32 devices in a mesh: gx: 4 (over z), gy: 8 (over y, x, core).
Axes of the slice: x: 2, y: 2, z: 4, core: 2. Of those that a mesh axis runs over, the one named last changes fastest.
Arguments:
- stored_vectors: bfloat16 [2, 16, 32, 4096], P(None, None, 'gx', 'gy'), may hold values from -4 to 4
- disorder: float32 [2, 32, 4096], P(None, 'gx', 'gy'), may hold values from -1.5 to 1.5
- vacancy: int32 [2, 32, 4096], P(None, 'gx', 'gy'), may hold values 0 or 1
- plan: int32 [32], replicated, may hold values from 0 to 31, as said below
Outputs:
- local_moments: float32 [4, 2, 32, 4096], P(None, None, 'gx', 'gy')
- trace_moments: float32 [4, 16], replicated
The draws below stay inside these ranges and needn't reach their ends.
Inputs may be any that keep to these rules, and one draw needn't show every extreme that they name: plan is a permutation of 0 to 31; stored block b is held by the device at gy index b // 4. The 4 lattice blocks of one device come from 4 different devices, and the 4 stored blocks of one device go to 4 different devices.
All inputs are finite; a program needn't handle non-finite values. No bound on the sum of `vacancy` on one device may be relied on, other than what follows from the above.
Results may differ from the reference program's by a relative error of at most 0.0003.
Values may be sent and summed in bfloat16 or wider, within the bound.
A program may use at most 64 MiB of HBM per device.

```python
import jax
import jax.numpy as jnp

BLOCK = 128
NB = 4
R = 16
TERMS = 4
LX = 32
LY = 4096
NBLK = 32


def draw_plan(key, part):
    devices = NBLK // NB
    key_tau, key_rho, key_offset, key_slot = jax.random.split(jax.random.fold_in(key, 7), 4)
    relabel = jax.random.permutation(key_tau, devices)
    order = jax.random.permutation(key_rho, devices)
    offsets = jax.random.permutation(key_offset, devices)[:NB]
    slots = jax.random.permutation(key_slot, NB)
    receiver = jnp.arange(devices)[:, None]
    within = jnp.arange(NB)[None, :]
    source = relabel[(order[receiver] + offsets[within]) % devices]
    return (source * NB + slots[within]).reshape(-1).astype(jnp.int32)


def place_ends(drawn, rng, low, high):
    extent = drawn.shape
    place = [jax.random.randint(jax.random.fold_in(rng, axis), (), 0, extent[axis]) for axis in range(len(extent))]
    drawn = drawn.at[tuple(place)].set(low)
    longest = extent.index(max(extent))
    place[longest] = (place[longest] + 1) % extent[longest]
    return drawn.at[tuple(place)].set(high)


def shard_levels(stream_key, shape, cuts, smallest, top_value):
    loudness, own = 1.0, jax.random.fold_in(stream_key, 6)
    for position, blocks in cuts:
        heights = jnp.exp(jax.random.uniform(jax.random.fold_in(own, position), (blocks,), jnp.float32, smallest / len(cuts), top_value / len(cuts)))
        loudness = loudness * jnp.repeat(heights, shape[position] // blocks).reshape([-1 if axis == position else 1 for axis in range(len(shape))])
    return loudness


def normal_values(own_key, extent, width, most, shards=(), kind=jnp.bfloat16):
    result = jax.random.normal(own_key, extent, jnp.float32) * width
    if len(shards) > 0:
        result = shard_levels(own_key, extent, shards, -0.22, 0.18) * result
    return jnp.clip(result, min=-most, max=most).astype(kind)


def setup_inputs(seed: int = 0) -> dict:
    key_list = jax.random.split(jax.random.key(seed), 5)
    stored_vectors = normal_values(key_list[0], (2, R, LX, LY), 1.0, 4.0, ((2, 4), (3, 8)))
    disorder = jnp.clip(jax.random.uniform(key_list[1], (2, LX, LY), jnp.float32, -1.5, 1.5) * shard_levels(key_list[1], (2, LX, LY), ((1, 4), (2, 8)), -0.4, 0.0), -1.5, 1.5)
    vacancy = place_ends((jax.random.randint(key_list[2], (2, LX, LY), 0, 10) < 9).astype(jnp.int32), jax.random.fold_in(key_list[2], 1), 0, 1)
    plan = draw_plan(jax.random.fold_in(key_list[4], 71), 0)
    return {"stored_vectors": stored_vectors, "disorder": disorder, "vacancy": vacancy, "plan": plan}


HOP_NEAR = 1.0
HOP_NEXT = 0.3
TWIST_COS = 0.4535961214255773
TWIST_SIN = 0.8912073600614354
SPREAD = 6.5
NEAR_A = ((0, 0), (-1, 0), (0, -1))
NEAR_B = ((0, 0), (1, 0), (0, 1))
SECOND = ((1, 0), (-1, 1), (0, -1))


def collect_sum(fetch, field, shifts):
    total = fetch(field, shifts[0])
    for shift in shifts[1:]:
        total = total + fetch(field, shift)
    return total


def hamilton(fetch, real, imag, onsite, keep):
    backs = tuple((-a, -b) for a, b in SECOND)
    out_real = []
    out_imag = []
    for sublat, chiral, bonds in ((0, 1.0, NEAR_A), (1, -1.0, NEAR_B)):
        other = 1 - sublat
        near_real = collect_sum(fetch, real[other], bonds)
        forward_real = collect_sum(fetch, real[sublat], SECOND)
        backward_real = collect_sum(fetch, real[sublat], backs)
        centre_real = fetch(real[sublat], (0, 0))
        mixed_real = TWIST_COS * (forward_real + backward_real)
        mixed_imag = chiral * TWIST_SIN * (forward_real - backward_real)
        level = onsite[sublat][None]
        if imag is None:
            result_imag = HOP_NEXT * mixed_imag
        else:
            near_imag = collect_sum(fetch, imag[other], bonds)
            forward_imag = collect_sum(fetch, imag[sublat], SECOND)
            backward_imag = collect_sum(fetch, imag[sublat], backs)
            centre_imag = fetch(imag[sublat], (0, 0))
            mixed_real = mixed_real - chiral * TWIST_SIN * (forward_imag - backward_imag)
            mixed_imag = mixed_imag + TWIST_COS * (forward_imag + backward_imag)
            result_imag = level * centre_imag - HOP_NEAR * near_imag + HOP_NEXT * mixed_imag
        result_real = level * centre_real - HOP_NEAR * near_real + HOP_NEXT * mixed_real
        factor = keep[sublat][None] / SPREAD
        out_real.append(result_real * factor)
        out_imag.append(result_imag * factor)
    return jnp.stack(out_real), jnp.stack(out_imag)


def rolled(field, shift):
    return jnp.roll(field, (-shift[0], -shift[1]), axis=(1, 2))


def reference(stored_vectors, disorder, vacancy, plan):
    blocks = stored_vectors.reshape(2, R, LX, NBLK, BLOCK)
    lattice = jnp.take(blocks, plan.astype(jnp.int32), axis=3).reshape(2, R, LX, LY)
    keep = vacancy.astype(jnp.float32)
    start = lattice.astype(jnp.float32) * keep[:, None]
    locals_list = []
    traces = []
    previous_real, previous_imag = start, None
    current_real, current_imag = hamilton(rolled, start, None, disorder, keep)
    locals_list.append(jnp.sum(start * current_real, axis=1) / R)
    traces.append(jnp.sum(start * current_real, axis=(0, 2, 3)) / (2 * LX * LY))
    for term in range(1, TERMS):
        image_real, image_imag = hamilton(rolled, current_real, current_imag, disorder, keep)
        next_real = 2.0 * image_real - previous_real
        if previous_imag is None:
            next_imag = 2.0 * image_imag
        else:
            next_imag = 2.0 * image_imag - previous_imag
        previous_real, previous_imag = current_real, current_imag
        current_real, current_imag = next_real, next_imag
        locals_list.append(jnp.sum(start * current_real, axis=1) / R)
        traces.append(jnp.sum(start * current_real, axis=(0, 2, 3)) / (2 * LX * LY))
    return jnp.stack(locals_list), jnp.stack(traces)
```

```python
import functools

import jax
import jax.numpy as jnp
from jax import lax
from jax.experimental import pallas as pl
from jax.experimental.pallas import tpu as pltpu
from jax.sharding import PartitionSpec as P

BLOCK = 128
TERMS = 4
HOP_NEXT = 0.3
TWIST_COS = 0.4535961214255773
TWIST_SIN = 0.8912073600614354
SPREAD = 6.5
HALO = TERMS
NEAR = 2
GROUP = 8
MESH = pl.DeviceIdType.MESH
F32 = jnp.float32
BF16 = jnp.bfloat16

WAYS = tuple((a, b) for a in (-1, 0, 1) for b in (-1, 0, 1) if (a, b) != (0, 0))


def rows_from(a, wide):
    if a == 0:
        return slice(HALO, HALO + wide)
    return slice(0, HALO) if a == 1 else slice(HALO + wide, 2 * HALO + wide)


def rows_to(a, wide):
    if a == 0:
        return slice(0, wide)
    return slice(wide - HALO, wide) if a == 1 else slice(0, HALO)


def program(
    nx, ny,
    plan_any, stored_any, disorder_any, vacancy_any,
    moments_ref, trace_ref,
    plan_ref, stored_ref, disorder_ref, vacancy_ref,
    turned, strips, send, edge_send, lattice, edge_own, edge_side,
    level_x, vac_x, site_edge, site_y, keep_ref, onsite, factor,
    real0, real1, real2, real3, imag1, imag2, imag3, sums, traces, part, parts,
    load_sem, a2a_send, a2a_recv, halo_send, halo_recv, site_send, site_recv, sum_send, sum_recv,
    *landing,
):
    gx, gy = lax.axis_index("gx"), lax.axis_index("gy")
    wide, long = disorder_ref.shape[1], disorder_ref.shape[2]
    halves = lattice.shape[0]
    vectors = halves * GROUP
    recv, edge_recv = landing[:halves], landing[halves:]
    extent = long + BLOCK
    blocks = long // BLOCK
    many = nx * ny
    cos, sin = HOP_NEXT * TWIST_COS, HOP_NEXT * TWIST_SIN

    def at(a, b):
        return (lax.rem(gx + a + nx, nx), lax.rem(gy + b + ny, ny))

    def copy(source, target, out_sem, in_sem, device):
        return pltpu.make_async_remote_copy(
            src_ref=source, dst_ref=target, send_sem=out_sem, recv_sem=in_sem,
            device_id=device, device_id_type=MESH,
        )

    loads = []
    for t, (source, target) in enumerate((
        (stored_any, stored_ref), (plan_any, plan_ref),
        (disorder_any, disorder_ref), (vacancy_any, vacancy_ref),
    )):
        loads.append(pltpu.make_async_copy(source, target, load_sem.at[t]))
        loads[-1].start()
    barrier = pltpu.get_barrier_semaphore()
    for i in range(1, many):
        pl.semaphore_signal(barrier, inc=1, device_id=at(i // ny, i % ny), device_id_type=MESH)
    traces[...] = jnp.zeros_like(traces)
    for load in loads:
        load.wait()

    lane = lax.broadcasted_iota(jnp.int32, (2 * GROUP, BLOCK), 1)
    place = ((lane + HALO) & (BLOCK - 1)) // (2 * HALO)
    is_last = (lane & HALO) != 0

    def turn(h):
        for k in range(blocks):
            piece = stored_ref[:, h * GROUP : (h + 1) * GROUP, :, k * BLOCK : (k + 1) * BLOCK]
            piece = piece.astype(F32).reshape(2 * GROUP, wide, BLOCK)
            piece = jnp.transpose(piece, (1, 0, 2))
            turned[h, k] = piece.astype(BF16)
            strip = piece[0]
            for x in range(1, wide):
                moved = pltpu.roll(piece[x], 2 * HALO * x, axis=1)
                strip = jnp.where(place == x, moved, strip)
            strips[h, k] = strip

    def mine(index):
        return plan_ref[lax.rem(index + ny * blocks, ny * blocks)] - gy * blocks

    def inside_mine(offset):
        return (offset >= 0) & (offset < blocks)

    picks = []
    for i in range(ny):
        target = lax.rem(gy + i, ny)
        pick = 0
        for j in range(blocks):
            offset = mine(target * blocks + j)
            pick = jnp.where(inside_mine(offset), offset, pick)
        left, right = mine(target * blocks - 1), mine(target * blocks + blocks)
        left = jnp.where(inside_mine(left), left, 0)
        right = jnp.where(inside_mine(right), right, 0)
        picks.append((pick, left, right))

    def fill(h):
        for i in range(1, ny):
            send[h, i] = turned[h, picks[i][0]]
        recv[h][gy] = turned[h, picks[0][0]]

    def fill_edges(h):
        def edge(i):
            return jnp.where(is_last, strips[h, picks[i][1]], strips[h, picks[i][2]]).astype(BF16)
        for i in range(1, ny):
            edge_send[h, i] = edge(i)
        edge_recv[h][gy] = edge(0)

    moves = [[] for _ in range(halves)]

    def start_blocks(h):
        for i in range(1, ny):
            move = copy(send.at[h, i], recv[h].at[gy], a2a_send.at[h, 0, i],
                        a2a_recv.at[h, 0, i], at(0, i))
            move.start()
            moves[h].append(move)

    def start_edges(h):
        for i in range(1, ny):
            move = copy(edge_send.at[h, i], edge_recv[h].at[gy], a2a_send.at[h, 1, i],
                        a2a_recv.at[h, 1, i], at(0, i))
            move.start()
            moves[h].append(move)

    turn(0)
    fill(0)
    fill_edges(0)
    pl.semaphore_wait(barrier, many - 1)
    start_blocks(0)
    start_edges(0)

    site_lane = lax.broadcasted_iota(jnp.int32, (2, wide, BLOCK), 2)
    low = site_lane < BLOCK // 2
    ends = []
    for own in (disorder_ref, vacancy_ref):
        ends.append(jnp.where(low, own[:, :, 0:BLOCK].astype(F32),
                              own[:, :, long - BLOCK : long].astype(F32)))
    shifted = pltpu.roll(ends[1], 4 * HALO, axis=2)
    near_end = ((site_lane + HALO) & (BLOCK - 1)) < 2 * HALO
    site_edge[...] = jnp.where(near_end, ends[0], shifted)
    low_shifted = ((site_lane - 4 * HALO) & (BLOCK - 1)) < BLOCK // 2
    sites = []

    def site_move(source, target, w, t):
        move = copy(source, target, site_send.at[w, t], site_recv.at[w, t], at(*WAYS[w]))
        move.start()
        sites.append(move)

    for w, (a, b) in enumerate(WAYS):
        if b == 0:
            site_move(disorder_ref, level_x.at[0 if a == -1 else 1], w, 0)
            site_move(vacancy_ref, vac_x.at[0 if a == -1 else 1], w, 1)
        else:
            site_move(site_edge, site_y.at[w], w, 0)

    for h in range(1, halves):
        turn(h)
        fill(h)
        start_blocks(h)
        fill_edges(h)
        start_edges(h)

    for move in sites:
        move.wait()
    for a in (-1, 0, 1):
        side = 0 if a == -1 else 1
        level = disorder_ref[...] if a == 0 else level_x[side]
        keep = (vacancy_ref[...] if a == 0 else vac_x[side]).astype(F32)
        right, left = site_y[WAYS.index((a, -1))], site_y[WAYS.index((a, 1))]
        edge = jnp.where(low, right, left)
        keep_edge = jnp.where(low_shifted, right, left)
        keep_edge = pltpu.roll(keep_edge, BLOCK - 4 * HALO, axis=2)
        kept, rows = rows_to(a, wide), rows_from(a, wide)
        for lanes, energy, present in (
            (slice(0, long), level, keep), (slice(long, extent), edge, keep_edge),
        ):
            energy, present = energy[:, kept], present[:, kept]
            scale = present * (1.0 / SPREAD)
            keep_ref[:, rows, lanes] = present
            factor[:, rows, lanes] = scale
            onsite[:, rows, lanes] = energy * scale

    def begin(h, first, last, edges):
        for x in range(first, last):
            rows = lattice[h, x].astype(F32)
            shift = (2 * BLOCK - 2 * HALO * edges[1] - 2 * HALO * (x - first)) % BLOCK
            edge = pltpu.roll(edges[0], shift, axis=1) if shift else edges[0]
            for s in range(2):
                mask = keep_ref[s, x : x + 1, :]
                own = slice(s * GROUP, (s + 1) * GROUP)
                real0[h, s, x, :, 0:long] = rows[own] * mask[:, 0:long]
                real0[h, s, x, :, long:] = edge[own] * mask[:, long:]

    halos = [{} for _ in range(halves)]

    def arrive(h):
        for move in moves[h]:
            move.wait()
        for k in range(blocks):
            source = plan_ref[gy * blocks + k] // blocks
            lattice[h, HALO : HALO + wide, :, k * BLOCK : (k + 1) * BLOCK] = recv[h][source]
        left = plan_ref[lax.rem(gy * blocks - 1 + ny * blocks, ny * blocks)] // blocks
        right = plan_ref[lax.rem(gy * blocks + blocks, ny * blocks)] // blocks
        edge = jnp.where(is_last, edge_recv[h][left].astype(F32), edge_recv[h][right].astype(F32))
        edge_own[h] = edge.astype(BF16)
        for part_of in ("near", "edge", "far"):
            for a in (1, -1):
                side = 0 if a == -1 else 1
                if part_of == "edge":
                    source, target = edge_own.at[h], edge_side.at[h, side]
                    slot = 2
                else:
                    near = part_of == "near"
                    slot = 0 if near else 1
                    if (a == 1) == near:
                        cut = slice(HALO - NEAR, HALO)
                    else:
                        cut = slice(0, NEAR)
                    rows_out, rows_in = rows_to(a, wide).start + HALO, rows_from(a, wide).start
                    source = lattice.at[h, rows_out + cut.start : rows_out + cut.stop]
                    target = lattice.at[h, rows_in + cut.start : rows_in + cut.stop]
                move = copy(source, target, halo_send.at[h, side, slot],
                            halo_recv.at[h, side, slot], at(a, 0))
                move.start()
                halos[h][part_of, a] = move
        begin(h, HALO, HALO + wide, (edge, 0))

    def back(value):
        return pltpu.roll(value, 1, axis=1)

    def ahead(value):
        return pltpu.roll(value, extent - 1, axis=1)

    def bond(r, i, first, second, chiral, want_imag):
        turn = chiral * sin
        out_real = cos * (r[first] + r[second])
        if i is not None:
            out_real = out_real - turn * (i[first] - i[second])
        out_imag = None
        if want_imag:
            out_imag = turn * (r[first] - r[second])
            if i is not None:
                out_imag = out_imag + cos * (i[first] + i[second])
        return out_real, out_imag

    reals_of = (real0, real1, real2, real3)
    imags_of = (None, imag1, imag2, imag3)

    def term(n, h, count, where, measure):
        if count <= 0:
            return
        cur_r, cur_i = reals_of[n - 1], imags_of[n - 1]
        complex_in, want_imag, keep_new = n > 1, n < TERMS, n < TERMS

        def row(x, measured):
            reals = [[cur_r[h, s, x + d] for d in (-1, 0, 1)] for s in range(2)]
            imags = [None, None]
            if complex_in:
                imags = [[cur_i[h, s, x + d] for d in (-1, 0, 1)] for s in range(2)]
            for s, chiral in ((0, 1.0), (1, -1.0)):
                r, i = reals[s], imags[s]
                other_r, other_i = reals[1 - s], imags[1 - s]
                here = bond(r, i, 2, 0, chiral, want_imag)
                behind = bond(r, i, 1, 2, chiral, want_imag)
                front = bond(r, i, 0, 1, chiral, want_imag)
                level = onsite[s, pl.ds(x, 1), :]
                scale = factor[s, pl.ds(x, 1), :]
                if n > 1:
                    level, scale = 2.0 * level, 2.0 * scale
                away = 0 if s == 0 else 2
                results = []
                for part_of in range(2 if want_imag else 1):
                    own, other = (r, other_r) if part_of == 0 else (i, other_i)
                    hop, prior, later = here[part_of], behind[part_of], front[part_of]
                    if other is not None:
                        hop = hop - (other[1] + other[away])
                        if s == 0:
                            prior = prior - other[1]
                        else:
                            later = later - other[1]
                    result = (hop + (back(prior) + ahead(later))) * scale
                    if own is not None:
                        result = result + level * own[1]
                    fields = reals_of if part_of == 0 else imags_of
                    if n > 1 and fields[n - 2] is not None:
                        result = result - fields[n - 2][h, s, x]
                    if keep_new:
                        fields[n][h, s, x] = result
                    results.append(result[:, :long])
                if measured is not None:
                    measured(s, x, real0[h, s, x, :, 0:long], results,
                             r[1][:, :long], None if i is None else i[1][:, :long])

        def plain(t, carry):
            row(where(t), None)
            return carry

        def middle(t, carry):
            def measured(s, x, start, results, now_r, now_i):
                product = start * results[0]
                total = product
                if h > 0:
                    total = sums[n - 1, s, x - HALO] + product
                if h < halves - 1:
                    sums[n - 1, s, x - HALO] = total
                else:
                    moments_ref[n - 1, s, pl.ds(x - HALO, 1), :] = (
                        jnp.sum(total, axis=0, keepdims=True) * (1.0 / vectors))
                if n == 1:
                    extra = ((0, product), (4, start * start))
                elif n == 2:
                    extra = (
                        (1, product),
                        (2, now_r * results[0] + now_i * results[1]),
                        (3, results[0] * results[0] + results[1] * results[1]),
                    )
                else:
                    extra = ()
                for slot, value in extra:
                    total = traces[h, slot]
                    for k in range(blocks):
                        total = total + value[:, k * BLOCK : (k + 1) * BLOCK]
                    traces[h, slot] = total

            row(where(t), measured)
            return carry

        lax.fori_loop(0, count, middle if measure else plain, 0)

    def inside(n, h):
        term(n, h, wide - 2 * n, lambda t: HALO + n + t, True)

    def border(n, h):
        term(n, h, 2 * n, lambda t: HALO + t + (wide - 2 * n) * (t // n), True)

    def halo_edges(h):
        return {a: edge_side[h, 0 if a == -1 else 1].astype(F32) for a in (1, -1)}

    def near_stage(h):
        for part_of in ("near", "edge"):
            for a in (1, -1):
                halos[h][part_of, a].wait()
        edges = halo_edges(h)
        begin(h, HALO - NEAR, HALO, (edges[1], wide - NEAR))
        begin(h, HALO + wide, HALO + wide + NEAR, (edges[-1], 0))
        term(1, h, 2, lambda t: HALO - 1 + t * (wide + 1), False)
        border(1, h)
        border(2, h)

    def far_stage(h):
        for a in (1, -1):
            halos[h]["far", a].wait()
        edges = halo_edges(h)
        begin(h, 0, HALO - NEAR, (edges[1], wide - HALO))
        begin(h, HALO + wide + NEAR, 2 * HALO + wide, (edges[-1], NEAR))
        term(1, h, 4, lambda t: 1 + t + (t // 2) * (wide + 2), False)
        term(2, h, 4, lambda t: 2 + t + (t // 2) * wide, False)
        term(3, h, 2, lambda t: 3 + t * (wide + 1), False)
        border(3, h)
        term(TERMS, h, wide, lambda t: HALO + t, True)

    small = lax.broadcasted_iota(jnp.int32, (GROUP, BLOCK), 1)
    slot_of = lax.broadcasted_iota(jnp.int32, (GROUP, BLOCK), 0)

    def gather_traces(h):
        out = jnp.zeros((GROUP, BLOCK), F32)
        for n in range(TERMS):
            value = traces[h, n]
            if n == 2:
                value = 2.0 * value - traces[h, 0]
            if n == 3:
                value = 2.0 * value - traces[h, 4]
            total = jnp.sum(value, axis=1, keepdims=True)
            out = jnp.where(small == slot_of + (n * vectors + h * GROUP), total, out)
        return jnp.sum(out, axis=0, keepdims=True)

    trace_row = jnp.zeros((1, BLOCK), F32)
    for h in range(halves):
        arrive(h)
        for n in range(1, TERMS):
            inside(n, h)
    for h in range(halves):
        near_stage(h)
        trace_row = trace_row + gather_traces(h)
        if h < halves - 1:
            far_stage(h)
    part[...] = trace_row
    me = gx * ny + gy
    parts[me] = trace_row
    sent = []
    for i in range(1, many):
        move = copy(part, parts.at[me], sum_send.at[i], sum_recv.at[i], at(i // ny, i % ny))
        move.start()
        sent.append(move)
    far_stage(halves - 1)
    for move in sent:
        move.wait()
    total = parts[0]
    for p in range(1, many):
        total = total + parts[p]
    sites_total = 2 * wide * nx * long * ny
    total = total * (1.0 / sites_total)
    for n in range(TERMS):
        turned_row = pltpu.roll(total, BLOCK - n * vectors, axis=1) if n else total
        trace_ref[n : n + 1, :] = turned_row[:, :vectors]


def local(nx, ny, stored_vectors, disorder, vacancy, plan):
    vectors, wide, long = stored_vectors.shape[1:]
    tall, extent = wide + 2 * HALO, long + BLOCK
    halves, blocks, pair = vectors // GROUP, long // BLOCK, 2 * GROUP
    dma = pltpu.SemaphoreType.DMA
    ways, many = len(WAYS), nx * ny
    field = pltpu.VMEM((halves, 2, tall, GROUP, extent), F32)
    return pl.pallas_call(
        functools.partial(program, nx, ny),
        out_shape=(
            pltpu.VMEM((TERMS, 2, wide, long), F32),
            pltpu.VMEM((TERMS, vectors), F32),
        ),
        in_specs=[pl.BlockSpec(memory_space=pl.ANY)] * 4,
        out_specs=(pl.BlockSpec(memory_space=pltpu.VMEM),) * 2,
        scratch_shapes=[
            pltpu.SMEM(plan.shape, jnp.int32),
            pltpu.VMEM(stored_vectors.shape, BF16),
            pltpu.VMEM(disorder.shape, F32),
            pltpu.VMEM(vacancy.shape, jnp.int32),
            pltpu.VMEM((halves, blocks, wide, pair, BLOCK), BF16),
            pltpu.VMEM((halves, blocks, pair, BLOCK), F32),
            pltpu.VMEM((halves, ny, wide, pair, BLOCK), BF16),
            pltpu.VMEM((halves, ny, pair, BLOCK), BF16),
            pltpu.VMEM((halves, tall, pair, long), BF16),
            pltpu.VMEM((halves, pair, BLOCK), BF16),
            pltpu.VMEM((halves, 2, pair, BLOCK), BF16),
            pltpu.VMEM((2, 2, wide, long), F32),
            pltpu.VMEM((2, 2, wide, long), jnp.int32),
            pltpu.VMEM((2, wide, BLOCK), F32),
            pltpu.VMEM((ways, 2, wide, BLOCK), F32),
        ]
        + [pltpu.VMEM((2, tall, extent), F32)] * 3
        + [field] * 7
        + [
            pltpu.VMEM((TERMS, 2, wide, GROUP, long), F32),
            pltpu.VMEM((halves, TERMS + 1, GROUP, BLOCK), F32),
            pltpu.VMEM((1, BLOCK), F32),
            pltpu.VMEM((many, 1, BLOCK), F32),
            dma((4,)),
            dma((halves, 2, ny)), dma((halves, 2, ny)),
            dma((halves, 2, 3)), dma((halves, 2, 3)),
            dma((ways, 2)), dma((ways, 2)),
            dma((many,)), dma((many,)),
        ]
        + [pltpu.VMEM((ny, wide, pair, BLOCK), BF16)] * halves
        + [pltpu.VMEM((ny, pair, BLOCK), BF16)] * halves,
        compiler_params=pltpu.CompilerParams(collective_id=0, has_side_effects=True),
        name="chebyshev",
    )(plan, stored_vectors, disorder, vacancy)


def solution(mesh):
    placed = (P(None, None, "gx", "gy"), P(None, "gx", "gy"), P(None, "gx", "gy"), P())
    return jax.shard_map(
        functools.partial(local, mesh.shape["gx"], mesh.shape["gy"]),
        mesh=mesh,
        in_specs=placed,
        out_specs=(P(None, None, "gx", "gy"), P()),
        check_vma=False,
    )
```

```python
import functools

import jax
import jax.numpy as jnp
from jax import lax
from jax.experimental import pallas as pl
from jax.experimental.pallas import tpu as pltpu
from jax.sharding import PartitionSpec as P

BLOCK = 128
TERMS = 4
HOP_NEXT = 0.3
TWIST_COS = 0.4535961214255773
TWIST_SIN = 0.8912073600614354
SPREAD = 6.5
HALO = TERMS
NEAR = 2
GROUP = 8
MESH = pl.DeviceIdType.MESH
F32 = jnp.float32
BF16 = jnp.bfloat16

def rows_from(a, wide):
    if a == 0:
        return slice(HALO, HALO + wide)
    return slice(0, HALO) if a == 1 else slice(HALO + wide, 2 * HALO + wide)


def rows_to(a, wide):
    if a == 0:
        return slice(0, wide)
    return slice(wide - HALO, wide) if a == 1 else slice(0, HALO)


def program(
    nx, ny,
    plan_any, stored_any, disorder_any, vacancy_any,
    moments_ref, trace_ref,
    plan_ref, stored_ref, disorder_ref, vacancy_ref,
    turned, strips, send, edge_send, edge_recv, lattice, edge_own, edge_side,
    site_send_x, site_x, site_edge, site_y, site_both, site_z, keep_ref, onsite, factor,
    real0, real1, real2, real3, imag1, imag2, imag3, sums, traces, part, parts,
    load_sem, a2a_send, a2a_recv, halo_send, halo_recv, site_send, site_recv, sum_send, sum_recv,
    *landing,
):
    gx, gy = lax.axis_index("gx"), lax.axis_index("gy")
    wide, long = disorder_ref.shape[1], disorder_ref.shape[2]
    halves = lattice.shape[0]
    vectors = halves * GROUP
    recv = landing
    extent = long + BLOCK
    blocks = long // BLOCK
    many = nx * ny
    cos, sin = HOP_NEXT * TWIST_COS, HOP_NEXT * TWIST_SIN

    def at(a, b):
        return (lax.rem(gx + a + nx, nx), lax.rem(gy + b + ny, ny))

    cores = 2 if ny % 2 == 0 else 1
    cols = 2 if (ny // cores) % 2 == 0 else 1
    lines = ny // (cores * cols)
    steps = [(r, c, u) for r in range(lines) for c in range(cols) for u in range(cores)]
    steps.sort(key=lambda step: -((step[0] != 0) + (step[1] != 0)))
    steps = [(0, 0, 0)] + [step for step in steps if step != (0, 0, 0)]

    def peer(i):
        r, c, u = steps[i]
        line = lax.rem(gy // (cores * cols) + r, lines)
        col = lax.rem(lax.rem(gy // cores, cols) + c, cols)
        return (line * cols + col) * cores + lax.rem(lax.rem(gy, cores) + u, cores)

    def copy(source, target, out_sem, in_sem, device):
        return pltpu.make_async_remote_copy(
            src_ref=source, dst_ref=target, send_sem=out_sem, recv_sem=in_sem,
            device_id=device, device_id_type=MESH,
        )

    loads = []
    for t, (source, target) in enumerate((
        (stored_any, stored_ref), (plan_any, plan_ref),
        (disorder_any, disorder_ref), (vacancy_any, vacancy_ref),
    )):
        loads.append(pltpu.make_async_copy(source, target, load_sem.at[t]))
        loads[-1].start()
    barrier = pltpu.get_barrier_semaphore()
    greeted = [(0, b) for b in range(1, ny)] + [(1, 0), (nx - 1, 0)]
    greeted += [(a, b) for a in range(3, nx - 2) for b in range(ny)]
    for a, b in greeted:
        pl.semaphore_signal(barrier, inc=1, device_id=at(a, b), device_id_type=MESH)
    traces[...] = jnp.zeros_like(traces)
    for load in loads:
        load.wait()

    lane = lax.broadcasted_iota(jnp.int32, (2 * GROUP, BLOCK), 1)
    place = ((lane + HALO) & (BLOCK - 1)) // (2 * HALO)
    is_last = (lane & HALO) != 0

    def turn(h):
        for k in range(blocks):
            piece = stored_ref[:, h * GROUP : (h + 1) * GROUP, :, k * BLOCK : (k + 1) * BLOCK]
            piece = piece.astype(F32).reshape(2 * GROUP, wide, BLOCK)
            piece = jnp.transpose(piece, (1, 0, 2))
            turned[h, k] = piece.astype(BF16)
            strip = strips[k] if h else piece[0]
            for x in range(0 if h else 1, wide):
                spot = h * wide + x
                moved = pltpu.roll(piece[x], 2 * HALO * spot, axis=1)
                strip = jnp.where(place == spot, moved, strip)
            strips[k] = strip

    def mine(index):
        return plan_ref[lax.rem(index + ny * blocks, ny * blocks)] - gy * blocks

    def inside_mine(offset):
        return (offset >= 0) & (offset < blocks)

    picks = []
    for i in range(ny):
        target = peer(i)
        pick = 0
        for j in range(blocks):
            offset = mine(target * blocks + j)
            pick = jnp.where(inside_mine(offset), offset, pick)
        left, right = mine(target * blocks - 1), mine(target * blocks + blocks)
        left = jnp.where(inside_mine(left), left, 0)
        right = jnp.where(inside_mine(right), right, 0)
        picks.append((pick, left, right))

    def fill(h):
        for i in range(1, ny):
            send[h, i] = turned[h, picks[i][0]]
        recv[h][gy] = turned[h, picks[0][0]]

    def fill_edges():
        def edge(i):
            return jnp.where(is_last, strips[picks[i][1]], strips[picks[i][2]]).astype(BF16)
        for i in range(1, ny):
            edge_send[i] = edge(i)
        edge_recv[gy] = edge(0)

    moves = [[] for _ in range(halves)]

    def start_blocks(h):
        for i in range(1, ny):
            move = copy(send.at[h, i], recv[h].at[gy], a2a_send.at[h, i],
                        a2a_recv.at[h, i], (gx, peer(i)))
            move.start()
            moves[h].append(move)

    def start_edges():
        for i in range(1, ny):
            move = copy(edge_send.at[i], edge_recv.at[gy], a2a_send.at[halves, i],
                        a2a_recv.at[halves, i], (gx, peer(i)))
            move.start()
            moves[0].append(move)

    turn(0)
    fill(0)
    site_lane = lax.broadcasted_iota(jnp.int32, (2, wide, BLOCK), 2)
    site_row = lax.broadcasted_iota(jnp.int32, (2, wide, BLOCK), 1)
    span = 4 * HALO
    low = site_lane < BLOCK // 2
    keep_own = vacancy_ref[...].astype(F32)
    ends = []
    for own in (disorder_ref[...], keep_own):
        ends.append(jnp.where(low, own[:, :, 0:BLOCK], own[:, :, long - BLOCK : long]))
    keep_end = jnp.where(low, pltpu.roll(ends[1], HALO, axis=2),
                         pltpu.roll(ends[1], BLOCK - HALO, axis=2))
    packed = jnp.where(((site_lane + HALO) & (BLOCK - 1)) < 2 * HALO, ends[0], keep_end)
    packed = pltpu.roll(packed, 0, axis=2, stride=span, stride_axis=1)
    packed = jnp.where(((site_lane + span // 2) & (BLOCK - 1)) // span == site_row, packed, 0.0)
    site_edge[...] = jnp.sum(packed, axis=1, keepdims=True)
    for a in (-1, 1):
        kept = rows_to(a, wide)
        rows = (disorder_ref[:, kept, :], keep_own[:, kept, :])
        site_send_x[0 if a == -1 else 1] = jnp.concatenate(rows, axis=1)
    sites = {}

    def site(name, source, target, w, device):
        sites[name] = copy(source, target, site_send.at[w], site_recv.at[w], device)
        sites[name].start()

    pl.semaphore_wait(barrier, len(greeted))
    for side, a in enumerate((-1, 1)):
        site(("x", a), site_send_x.at[side], site_x.at[side], side, at(a, 0))
        site(("y", a), site_edge, site_y.at[side], 2 + side, at(0, a))
    start_blocks(0)

    for h in range(1, halves):
        turn(h)
    fill_edges()
    start_edges()
    for h in range(1, halves):
        fill(h)
        for move in moves[h - 1][: ny - 1]:
            move.wait_send()
        start_blocks(h)

    short = lax.broadcasted_iota(jnp.int32, (2, 1, BLOCK), 2)

    def site_ends(a, both):
        rows, kept = rows_from(a, wide), rows_to(a, wide)
        for x in range(rows.start, rows.stop):
            shift = 2 * BLOCK - span * (x - rows.start + kept.start)
            energy = pltpu.roll(both, shift % BLOCK, axis=2)
            present = jnp.where(short < BLOCK // 2,
                                pltpu.roll(both, (shift - HALO) % BLOCK, axis=2),
                                pltpu.roll(both, (shift + HALO) % BLOCK, axis=2))
            scale = present * (1.0 / SPREAD)
            keep_ref[:, x : x + 1, long:] = present
            factor[:, x : x + 1, long:] = scale
            onsite[:, x : x + 1, long:] = energy * scale

    def site_rows(a, energy, present):
        rows = rows_from(a, wide)
        scale = present * (1.0 / SPREAD)
        keep_ref[:, rows, 0:long] = present
        factor[:, rows, 0:long] = scale
        onsite[:, rows, 0:long] = energy * scale

    site_rows(0, disorder_ref[...], keep_own)
    for a in (-1, 1):
        sites["y", a].wait()
    site_both[...] = jnp.where((short & (span // 2)) == 0, site_y[0], site_y[1])
    for side, a in enumerate((-1, 1)):
        site(("z", a), site_both, site_z.at[side], 4 + side, at(a, 0))
    site_ends(0, site_both[...])
    for side, a in enumerate((-1, 1)):
        sites["x", a].wait()
        site_rows(a, site_x[side, :, 0:HALO], site_x[side, :, HALO:])

    def far_sites():
        for side, a in enumerate((-1, 1)):
            sites["z", a].wait()
            site_ends(a, site_z[side])

    def begin(h, first, last, edges):
        for x in range(first, last):
            rows = lattice[h, x].astype(F32)
            shift = (-2 * HALO * (h * wide + edges[1] + x - first)) % BLOCK
            edge = pltpu.roll(edges[0], shift, axis=1) if shift else edges[0]
            for s in range(2):
                mask = keep_ref[s, x : x + 1, :]
                own = slice(s * GROUP, (s + 1) * GROUP)
                real0[h, s, x, :, 0:long] = rows[own] * mask[:, 0:long]
                real0[h, s, x, :, long:] = edge[own] * mask[:, long:]

    halos = [{} for _ in range(halves)]

    def halo(h, name, a, source, target, slot):
        side = 0 if a == -1 else 1
        halos[h][name, a] = copy(source, target, halo_send.at[h, side, slot],
                                 halo_recv.at[h, side, slot], at(a, 0))
        halos[h][name, a].start()

    def own_edge():
        left = plan_ref[lax.rem(gy * blocks - 1 + ny * blocks, ny * blocks)] // blocks
        right = plan_ref[lax.rem(gy * blocks + blocks, ny * blocks)] // blocks
        return jnp.where(is_last, edge_recv[left].astype(F32), edge_recv[right].astype(F32))

    def arrive(h):
        for j, move in enumerate(moves[h]):
            move.wait_recv()
            if h == halves - 1 or j >= ny - 1:
                move.wait_send()
        for k in range(blocks):
            source = plan_ref[gy * blocks + k] // blocks
            lattice[h, HALO : HALO + wide, :, k * BLOCK : (k + 1) * BLOCK] = recv[h][source]
        for name in ("near", "far"):
            for a in (1, -1):
                last = (a == 1) == (name == "near")
                cut = slice(HALO - NEAR, HALO) if last else slice(0, NEAR)
                rows_out, rows_in = rows_to(a, wide).start + HALO, rows_from(a, wide).start
                source = lattice.at[h, rows_out + cut.start : rows_out + cut.stop]
                target = lattice.at[h, rows_in + cut.start : rows_in + cut.stop]
                halo(h, name, a, source, target, 0 if name == "near" else 1)
            if h == 0 and name == "near":
                edge_own[...] = own_edge().astype(BF16)
                for a in (1, -1):
                    halo(0, "edge", a, edge_own, edge_side.at[0 if a == -1 else 1], 2)
        begin(h, HALO, HALO + wide, (own_edge(), 0))

    def back(value):
        return pltpu.roll(value, 1, axis=1)

    def ahead(value):
        return pltpu.roll(value, extent - 1, axis=1)

    def bond(r, i, first, second, chiral, want_imag):
        turn = chiral * sin
        out_real = cos * (r[first] + r[second])
        if i is not None:
            out_real = out_real - turn * (i[first] - i[second])
        out_imag = None
        if want_imag:
            out_imag = turn * (r[first] - r[second])
            if i is not None:
                out_imag = out_imag + cos * (i[first] + i[second])
        return out_real, out_imag

    reals_of = (real0, real1, real2, real3)
    imags_of = (None, imag1, imag2, imag3)

    def term(n, h, count, where, measure):
        if count <= 0:
            return
        cur_r, cur_i = reals_of[n - 1], imags_of[n - 1]
        complex_in, want_imag, keep_new = n > 1, n < TERMS, n < TERMS

        def row(x, measured):
            reals = [[cur_r[h, s, x + d] for d in (-1, 0, 1)] for s in range(2)]
            imags = [None, None]
            if complex_in:
                imags = [[cur_i[h, s, x + d] for d in (-1, 0, 1)] for s in range(2)]
            for s, chiral in ((0, 1.0), (1, -1.0)):
                r, i = reals[s], imags[s]
                other_r, other_i = reals[1 - s], imags[1 - s]
                here = bond(r, i, 2, 0, chiral, want_imag)
                behind = bond(r, i, 1, 2, chiral, want_imag)
                front = bond(r, i, 0, 1, chiral, want_imag)
                level = onsite[s, pl.ds(x, 1), :]
                scale = factor[s, pl.ds(x, 1), :]
                if n > 1:
                    level, scale = 2.0 * level, 2.0 * scale
                away = 0 if s == 0 else 2
                results = []
                for part_of in range(2 if want_imag else 1):
                    own, other = (r, other_r) if part_of == 0 else (i, other_i)
                    hop, prior, later = here[part_of], behind[part_of], front[part_of]
                    if other is not None:
                        hop = hop - (other[1] + other[away])
                        if s == 0:
                            prior = prior - other[1]
                        else:
                            later = later - other[1]
                    result = (hop + (back(prior) + ahead(later))) * scale
                    if own is not None:
                        result = result + level * own[1]
                    fields = reals_of if part_of == 0 else imags_of
                    if n > 1 and fields[n - 2] is not None:
                        result = result - fields[n - 2][h, s, x]
                    if keep_new:
                        fields[n][h, s, x] = result
                    results.append(result[:, :long])
                if measured is not None:
                    measured(s, x, real0[h, s, x, :, 0:long], results,
                             r[1][:, :long], None if i is None else i[1][:, :long])

        def plain(t, carry):
            row(where(t), None)
            return carry

        def middle(t, carry):
            def measured(s, x, start, results, now_r, now_i):
                product = start * results[0]
                total = product
                if h > 0:
                    total = sums[n - 1, s, x - HALO] + product
                if h < halves - 1:
                    sums[n - 1, s, x - HALO] = total
                else:
                    moments_ref[n - 1, s, pl.ds(x - HALO, 1), :] = (
                        jnp.sum(total, axis=0, keepdims=True) * (1.0 / vectors))
                if n == 1:
                    extra = ((0, product), (4, start * start))
                elif n == 2:
                    extra = (
                        (1, product),
                        (2, now_r * results[0] + now_i * results[1]),
                        (3, results[0] * results[0] + results[1] * results[1]),
                    )
                else:
                    extra = ()
                for slot, value in extra:
                    total = traces[h, slot]
                    for k in range(blocks):
                        total = total + value[:, k * BLOCK : (k + 1) * BLOCK]
                    traces[h, slot] = total

            row(where(t), measured)
            return carry

        lax.fori_loop(0, count, middle if measure else plain, 0)

    def inside(n, h):
        term(n, h, wide - 2 * n, lambda t: HALO + n + t, True)

    def border(n, h):
        term(n, h, 2 * n, lambda t: HALO + t + (wide - 2 * n) * (t // n), True)

    def halo_edges():
        return {a: edge_side[0 if a == -1 else 1].astype(F32) for a in (1, -1)}

    def near_stage(h):
        for a in (1, -1):
            if h == 0:
                halos[h]["edge", a].wait()
            halos[h]["near", a].wait()
        edges = halo_edges()
        begin(h, HALO - NEAR, HALO, (edges[1], wide - NEAR))
        begin(h, HALO + wide, HALO + wide + NEAR, (edges[-1], 0))
        term(1, h, 2, lambda t: HALO - 1 + t * (wide + 1), False)
        border(1, h)
        border(2, h)

    def far_stage(h):
        for a in (1, -1):
            halos[h]["far", a].wait()
        edges = halo_edges()
        begin(h, 0, HALO - NEAR, (edges[1], wide - HALO))
        begin(h, HALO + wide + NEAR, 2 * HALO + wide, (edges[-1], NEAR))
        term(1, h, 4, lambda t: 1 + t + (t // 2) * (wide + 2), False)
        term(2, h, 4, lambda t: 2 + t + (t // 2) * wide, False)
        term(3, h, 2, lambda t: 3 + t * (wide + 1), False)
        border(3, h)
        term(TERMS, h, wide, lambda t: HALO + t, True)

    small = lax.broadcasted_iota(jnp.int32, (GROUP, BLOCK), 1)
    slot_of = lax.broadcasted_iota(jnp.int32, (GROUP, BLOCK), 0)

    def gather_traces(h):
        out = jnp.zeros((GROUP, BLOCK), F32)
        for n in range(TERMS):
            value = traces[h, n]
            if n == 2:
                value = 2.0 * value - traces[h, 0]
            if n == 3:
                value = 2.0 * value - traces[h, 4]
            total = jnp.sum(value, axis=1, keepdims=True)
            out = jnp.where(small == slot_of + (n * vectors + h * GROUP), total, out)
        return jnp.sum(out, axis=0, keepdims=True)

    trace_row = jnp.zeros((1, BLOCK), F32)
    for h in range(halves):
        arrive(h)
        for n in range(1, TERMS):
            inside(n, h)
    far_sites()
    for h in range(halves):
        near_stage(h)
        trace_row = trace_row + gather_traces(h)
    part[...] = trace_row
    me = gx * ny + gy
    parts[me] = trace_row
    sent = []
    for i in range(1, many):
        move = copy(part, parts.at[me], sum_send.at[i], sum_recv.at[i], at(i // ny, i % ny))
        move.start()
        sent.append(move)
    for h in range(halves):
        far_stage(h)
    for move in sent:
        move.wait()
    total = parts[0]
    for p in range(1, many):
        total = total + parts[p]
    sites_total = 2 * wide * nx * long * ny
    total = total * (1.0 / sites_total)
    for n in range(TERMS):
        turned_row = pltpu.roll(total, BLOCK - n * vectors, axis=1) if n else total
        trace_ref[n : n + 1, :] = turned_row[:, :vectors]


def local(nx, ny, stored_vectors, disorder, vacancy, plan):
    vectors, wide, long = stored_vectors.shape[1:]
    tall, extent = wide + 2 * HALO, long + BLOCK
    halves, blocks, pair = vectors // GROUP, long // BLOCK, 2 * GROUP
    dma = pltpu.SemaphoreType.DMA
    many = nx * ny
    field = pltpu.VMEM((halves, 2, tall, GROUP, extent), F32)
    return pl.pallas_call(
        functools.partial(program, nx, ny),
        out_shape=(
            pltpu.VMEM((TERMS, 2, wide, long), F32),
            pltpu.VMEM((TERMS, vectors), F32),
        ),
        in_specs=[pl.BlockSpec(memory_space=pl.ANY)] * 4,
        out_specs=(pl.BlockSpec(memory_space=pltpu.VMEM),) * 2,
        scratch_shapes=[
            pltpu.SMEM(plan.shape, jnp.int32),
            pltpu.VMEM(stored_vectors.shape, BF16),
            pltpu.VMEM(disorder.shape, F32),
            pltpu.VMEM(vacancy.shape, jnp.int32),
            pltpu.VMEM((halves, blocks, wide, pair, BLOCK), BF16),
            pltpu.VMEM((blocks, pair, BLOCK), F32),
            pltpu.VMEM((halves, ny, wide, pair, BLOCK), BF16),
            pltpu.VMEM((ny, pair, BLOCK), BF16),
            pltpu.VMEM((ny, pair, BLOCK), BF16),
            pltpu.VMEM((halves, tall, pair, long), BF16),
            pltpu.VMEM((pair, BLOCK), BF16),
            pltpu.VMEM((2, pair, BLOCK), BF16),
            pltpu.VMEM((2, 2, 2 * HALO, long), F32),
            pltpu.VMEM((2, 2, 2 * HALO, long), F32),
            pltpu.VMEM((2, 1, BLOCK), F32),
            pltpu.VMEM((2, 2, 1, BLOCK), F32),
            pltpu.VMEM((2, 1, BLOCK), F32),
            pltpu.VMEM((2, 2, 1, BLOCK), F32),
        ]
        + [pltpu.VMEM((2, tall, extent), F32)] * 3
        + [field] * 7
        + [
            pltpu.VMEM((TERMS, 2, wide, GROUP, long), F32),
            pltpu.VMEM((halves, TERMS + 1, GROUP, BLOCK), F32),
            pltpu.VMEM((1, BLOCK), F32),
            pltpu.VMEM((many, 1, BLOCK), F32),
            dma((4,)),
            dma((halves + 1, ny)), dma((halves + 1, ny)),
            dma((halves, 2, 3)), dma((halves, 2, 3)),
            dma((6,)), dma((6,)),
            dma((many,)), dma((many,)),
        ]
        + [pltpu.VMEM((ny, wide, pair, BLOCK), BF16)] * halves,
        compiler_params=pltpu.CompilerParams(collective_id=0, has_side_effects=True),
        name="chebyshev",
    )(plan, stored_vectors, disorder, vacancy)


def solution(mesh):
    placed = (P(None, None, "gx", "gy"), P(None, "gx", "gy"), P(None, "gx", "gy"), P())
    return jax.shard_map(
        functools.partial(local, mesh.shape["gx"], mesh.shape["gy"]),
        mesh=mesh,
        in_specs=placed,
        out_specs=(P(None, None, "gx", "gy"), P()),
        check_vma=False,
    )
```

```python
import functools

import jax
import jax.numpy as jnp
from jax import lax
from jax.experimental import pallas as pl
from jax.experimental.pallas import tpu as pltpu
from jax.sharding import PartitionSpec as P

BLOCK = 128
TERMS = 4
HOP_NEXT = 0.3
TWIST_COS = 0.4535961214255773
TWIST_SIN = 0.8912073600614354
SPREAD = 6.5
HALO = TERMS
NEAR = 2
GROUP = 8
MESH = pl.DeviceIdType.MESH
F32 = jnp.float32
BF16 = jnp.bfloat16

def rows_from(a, wide):
    if a == 0:
        return slice(HALO, HALO + wide)
    return slice(0, HALO) if a == 1 else slice(HALO + wide, 2 * HALO + wide)


def rows_to(a, wide):
    if a == 0:
        return slice(0, wide)
    return slice(wide - HALO, wide) if a == 1 else slice(0, HALO)


def program(
    nx, ny,
    plan_any, stored_any, disorder_any, vacancy_any,
    moments_ref, trace_ref,
    plan_ref, stored_ref, disorder_ref, vacancy_ref,
    turned, strips, send, edge_send, edge_recv, lattice, edge_own, edge_side,
    site_send_x, site_x, site_edge, site_y, site_both, site_z, keep_ref, onsite, factor,
    real0, real1, real2, real3, imag1, imag2, imag3, sums, traces, part, parts,
    load_sem, a2a_send, a2a_recv, halo_send, halo_recv, site_send, site_recv, sum_send, sum_recv, token,
    *landing,
):
    gx, gy = lax.axis_index("gx"), lax.axis_index("gy")
    wide, long = disorder_ref.shape[1], disorder_ref.shape[2]
    halves = lattice.shape[0]
    vectors = halves * GROUP
    recv = landing
    extent = long + BLOCK
    blocks = long // BLOCK
    many = nx * ny
    cos, sin = HOP_NEXT * TWIST_COS, HOP_NEXT * TWIST_SIN

    def at(a, b):
        return (lax.rem(gx + a + nx, nx), lax.rem(gy + b + ny, ny))

    cores = 2 if ny % 2 == 0 else 1
    cols = 2 if (ny // cores) % 2 == 0 else 1
    lines = ny // (cores * cols)
    steps = [(r, c, u) for r in range(lines) for c in range(cols) for u in range(cores)]
    steps.sort(key=lambda step: -((step[0] != 0) + (step[1] != 0)))
    steps = [(0, 0, 0)] + [step for step in steps if step != (0, 0, 0)]

    def peer(i):
        r, c, u = steps[i]
        line = lax.rem(gy // (cores * cols) + r, lines)
        col = lax.rem(lax.rem(gy // cores, cols) + c, cols)
        return (line * cols + col) * cores + lax.rem(lax.rem(gy, cores) + u, cores)

    def copy(source, target, out_sem, in_sem, device):
        return pltpu.make_async_remote_copy(
            src_ref=source, dst_ref=target, send_sem=out_sem, recv_sem=in_sem,
            device_id=device, device_id_type=MESH,
        )

    loads = []
    for t, (source, target) in enumerate((
        (stored_any, stored_ref), (plan_any, plan_ref),
        (disorder_any, disorder_ref), (vacancy_any, vacancy_ref),
    )):
        loads.append(pltpu.make_async_copy(source, target, load_sem.at[t]))
        loads[-1].start()
    barrier = pltpu.get_barrier_semaphore()
    linked = {-1: gx > 0, 1: gx < nx - 1}

    def greet(sem, a, b):
        pl.semaphore_signal(sem, inc=1, device_id=at(a, b), device_id_type=MESH)

    for b in range(1, ny):
        greet(barrier, 0, b)
    for a in (-1, 1):
        pl.when(linked[a])(functools.partial(greet, barrier, a, 0))
    entered = ny - 1 + linked[-1].astype(jnp.int32) + linked[1].astype(jnp.int32)

    def pass_on(step):
        for side, a in enumerate((-1, 1)):
            pl.when(linked[a])(functools.partial(greet, token.at[step, 1 - side], a, 0))

    def hear(step):
        for side, a in enumerate((-1, 1)):
            pl.when(linked[a])(functools.partial(pl.semaphore_wait, token.at[step, side], 1))

    traces[...] = jnp.zeros_like(traces)
    for load in loads:
        load.wait()

    lane = lax.broadcasted_iota(jnp.int32, (2 * GROUP, BLOCK), 1)
    place = ((lane + HALO) & (BLOCK - 1)) // (2 * HALO)
    is_last = (lane & HALO) != 0

    def turn(h):
        for k in range(blocks):
            piece = stored_ref[:, h * GROUP : (h + 1) * GROUP, :, k * BLOCK : (k + 1) * BLOCK]
            piece = piece.astype(F32).reshape(2 * GROUP, wide, BLOCK)
            piece = jnp.transpose(piece, (1, 0, 2))
            turned[h, k] = piece.astype(BF16)
            strip = strips[k] if h else piece[0]
            for x in range(0 if h else 1, wide):
                spot = h * wide + x
                moved = pltpu.roll(piece[x], 2 * HALO * spot, axis=1)
                strip = jnp.where(place == spot, moved, strip)
            strips[k] = strip

    def mine(index):
        return plan_ref[lax.rem(index + ny * blocks, ny * blocks)] - gy * blocks

    def inside_mine(offset):
        return (offset >= 0) & (offset < blocks)

    picks = []
    for i in range(ny):
        target = peer(i)
        pick = 0
        for j in range(blocks):
            offset = mine(target * blocks + j)
            pick = jnp.where(inside_mine(offset), offset, pick)
        left, right = mine(target * blocks - 1), mine(target * blocks + blocks)
        left = jnp.where(inside_mine(left), left, 0)
        right = jnp.where(inside_mine(right), right, 0)
        picks.append((pick, left, right))

    def fill(h):
        for i in range(1, ny):
            send[h, i] = turned[h, picks[i][0]]
        recv[h][gy] = turned[h, picks[0][0]]

    def fill_edges():
        def edge(i):
            return jnp.where(is_last, strips[picks[i][1]], strips[picks[i][2]]).astype(BF16)
        for i in range(1, ny):
            edge_send[i] = edge(i)
        edge_recv[gy] = edge(0)

    moves = [[] for _ in range(halves)]

    def start_blocks(h):
        for i in range(1, ny):
            move = copy(send.at[h, i], recv[h].at[gy], a2a_send.at[h, i],
                        a2a_recv.at[h, i], (gx, peer(i)))
            move.start()
            moves[h].append(move)

    def start_edges():
        for i in range(1, ny):
            move = copy(edge_send.at[i], edge_recv.at[gy], a2a_send.at[halves, i],
                        a2a_recv.at[halves, i], (gx, peer(i)))
            move.start()
            moves[0].append(move)

    turn(0)
    fill(0)
    site_lane = lax.broadcasted_iota(jnp.int32, (2, wide, BLOCK), 2)
    site_row = lax.broadcasted_iota(jnp.int32, (2, wide, BLOCK), 1)
    span = 4 * HALO
    low = site_lane < BLOCK // 2
    keep_own = vacancy_ref[...].astype(F32)
    ends = []
    for own in (disorder_ref[...], keep_own):
        ends.append(jnp.where(low, own[:, :, 0:BLOCK], own[:, :, long - BLOCK : long]))
    keep_end = jnp.where(low, pltpu.roll(ends[1], HALO, axis=2),
                         pltpu.roll(ends[1], BLOCK - HALO, axis=2))
    packed = jnp.where(((site_lane + HALO) & (BLOCK - 1)) < 2 * HALO, ends[0], keep_end)
    packed = pltpu.roll(packed, 0, axis=2, stride=span, stride_axis=1)
    packed = jnp.where(((site_lane + span // 2) & (BLOCK - 1)) // span == site_row, packed, 0.0)
    site_edge[...] = jnp.sum(packed, axis=1, keepdims=True)
    for a in (-1, 1):
        kept = rows_to(a, wide)
        rows = (disorder_ref[:, kept, :], keep_own[:, kept, :])
        site_send_x[0 if a == -1 else 1] = jnp.concatenate(rows, axis=1)
    sites = {}

    def site(name, source, target, w, device, when=None):
        sites[name] = copy(source, target, site_send.at[w], site_recv.at[w], device)
        if when is None:
            sites[name].start()
        else:
            pl.when(when)(sites[name].start)

    pl.semaphore_wait(barrier, entered)
    pass_on(0)
    for side, a in enumerate((-1, 1)):
        site(("x", a), site_send_x.at[side], site_x.at[side], side, at(a, 0), linked[a])
        site(("y", a), site_edge, site_y.at[side], 2 + side, at(0, a))
    start_blocks(0)

    for h in range(1, halves):
        turn(h)
    fill_edges()
    start_edges()
    def token_round(step):
        hear(step)
        if step < nx - 3:
            pass_on(step + 1)

    for step in range(nx - 3):
        token_round(step)
    for h in range(1, halves):
        fill(h)
        for move in moves[h - 1][: ny - 1]:
            move.wait_send()
        start_blocks(h)
    token_round(nx - 3)
    for a in (-1, 1):
        pl.when(~linked[a])(sites["x", a].start)

    short = lax.broadcasted_iota(jnp.int32, (2, 1, BLOCK), 2)

    def site_ends(a, both):
        rows, kept = rows_from(a, wide), rows_to(a, wide)
        for x in range(rows.start, rows.stop):
            shift = 2 * BLOCK - span * (x - rows.start + kept.start)
            energy = pltpu.roll(both, shift % BLOCK, axis=2)
            present = jnp.where(short < BLOCK // 2,
                                pltpu.roll(both, (shift - HALO) % BLOCK, axis=2),
                                pltpu.roll(both, (shift + HALO) % BLOCK, axis=2))
            scale = present * (1.0 / SPREAD)
            keep_ref[:, x : x + 1, long:] = present
            factor[:, x : x + 1, long:] = scale
            onsite[:, x : x + 1, long:] = energy * scale

    def site_rows(a, energy, present):
        rows = rows_from(a, wide)
        scale = present * (1.0 / SPREAD)
        keep_ref[:, rows, 0:long] = present
        factor[:, rows, 0:long] = scale
        onsite[:, rows, 0:long] = energy * scale

    site_rows(0, disorder_ref[...], keep_own)
    for a in (-1, 1):
        sites["y", a].wait()
    site_both[...] = jnp.where((short & (span // 2)) == 0, site_y[0], site_y[1])
    for side, a in enumerate((-1, 1)):
        site(("z", a), site_both, site_z.at[side], 4 + side, at(a, 0))
    site_ends(0, site_both[...])

    def far_sites():
        for side, a in enumerate((-1, 1)):
            sites["x", a].wait()
            site_rows(a, site_x[side, :, 0:HALO], site_x[side, :, HALO:])
            sites["z", a].wait()
            site_ends(a, site_z[side])

    def begin(h, first, last, edges):
        for x in range(first, last):
            rows = lattice[h, x].astype(F32)
            shift = (-2 * HALO * (h * wide + edges[1] + x - first)) % BLOCK
            edge = pltpu.roll(edges[0], shift, axis=1) if shift else edges[0]
            for s in range(2):
                mask = keep_ref[s, x : x + 1, :]
                own = slice(s * GROUP, (s + 1) * GROUP)
                real0[h, s, x, :, 0:long] = rows[own] * mask[:, 0:long]
                real0[h, s, x, :, long:] = edge[own] * mask[:, long:]

    halos = [{} for _ in range(halves)]

    def halo(h, name, a, source, target, slot):
        side = 0 if a == -1 else 1
        halos[h][name, a] = copy(source, target, halo_send.at[h, side, slot],
                                 halo_recv.at[h, side, slot], at(a, 0))
        halos[h][name, a].start()

    def own_edge():
        left = plan_ref[lax.rem(gy * blocks - 1 + ny * blocks, ny * blocks)] // blocks
        right = plan_ref[lax.rem(gy * blocks + blocks, ny * blocks)] // blocks
        return jnp.where(is_last, edge_recv[left].astype(F32), edge_recv[right].astype(F32))

    def send_rows(h, name):
        for a in (1, -1):
            last = (a == 1) == (name == "near")
            cut = slice(HALO - NEAR, HALO) if last else slice(0, NEAR)
            rows_out, rows_in = rows_to(a, wide).start + HALO, rows_from(a, wide).start
            source = lattice.at[h, rows_out + cut.start : rows_out + cut.stop]
            target = lattice.at[h, rows_in + cut.start : rows_in + cut.stop]
            halo(h, name, a, source, target, 0 if name == "near" else 1)

    def arrive(h):
        for j, move in enumerate(moves[h]):
            move.wait_recv()
            if h == halves - 1 or j >= ny - 1:
                move.wait_send()
        for k in range(blocks):
            source = plan_ref[gy * blocks + k] // blocks
            lattice[h, HALO : HALO + wide, :, k * BLOCK : (k + 1) * BLOCK] = recv[h][source]
        send_rows(h, "near")
        if h == 0:
            edge_own[...] = own_edge().astype(BF16)
            for a in (1, -1):
                halo(0, "edge", a, edge_own, edge_side.at[0 if a == -1 else 1], 2)
        begin(h, HALO, HALO + wide, (own_edge(), 0))

    def back(value):
        return pltpu.roll(value, 1, axis=1)

    def ahead(value):
        return pltpu.roll(value, extent - 1, axis=1)

    def bond(r, i, first, second, chiral, want_imag):
        turn = chiral * sin
        out_real = cos * (r[first] + r[second])
        if i is not None:
            out_real = out_real - turn * (i[first] - i[second])
        out_imag = None
        if want_imag:
            out_imag = turn * (r[first] - r[second])
            if i is not None:
                out_imag = out_imag + cos * (i[first] + i[second])
        return out_real, out_imag

    reals_of = (real0, real1, real2, real3)
    imags_of = (None, imag1, imag2, imag3)

    def term(n, h, count, where, measure):
        if count <= 0:
            return
        cur_r, cur_i = reals_of[n - 1], imags_of[n - 1]
        complex_in, want_imag, keep_new = n > 1, n < TERMS, n < TERMS

        def row(x, measured):
            reals = [[cur_r[h, s, x + d] for d in (-1, 0, 1)] for s in range(2)]
            imags = [None, None]
            if complex_in:
                imags = [[cur_i[h, s, x + d] for d in (-1, 0, 1)] for s in range(2)]
            for s, chiral in ((0, 1.0), (1, -1.0)):
                r, i = reals[s], imags[s]
                other_r, other_i = reals[1 - s], imags[1 - s]
                here = bond(r, i, 2, 0, chiral, want_imag)
                behind = bond(r, i, 1, 2, chiral, want_imag)
                front = bond(r, i, 0, 1, chiral, want_imag)
                level = onsite[s, pl.ds(x, 1), :]
                scale = factor[s, pl.ds(x, 1), :]
                if n > 1:
                    level, scale = 2.0 * level, 2.0 * scale
                away = 0 if s == 0 else 2
                results = []
                for part_of in range(2 if want_imag else 1):
                    own, other = (r, other_r) if part_of == 0 else (i, other_i)
                    hop, prior, later = here[part_of], behind[part_of], front[part_of]
                    if other is not None:
                        hop = hop - (other[1] + other[away])
                        if s == 0:
                            prior = prior - other[1]
                        else:
                            later = later - other[1]
                    result = (hop + (back(prior) + ahead(later))) * scale
                    if own is not None:
                        result = result + level * own[1]
                    fields = reals_of if part_of == 0 else imags_of
                    if n > 1 and fields[n - 2] is not None:
                        result = result - fields[n - 2][h, s, x]
                    if keep_new:
                        fields[n][h, s, x] = result
                    results.append(result[:, :long])
                if measured is not None:
                    measured(s, x, real0[h, s, x, :, 0:long], results,
                             r[1][:, :long], None if i is None else i[1][:, :long])

        def plain(t, carry):
            row(where(t), None)
            return carry

        def middle(t, carry):
            def measured(s, x, start, results, now_r, now_i):
                product = start * results[0]
                total = product
                if h > 0:
                    total = sums[n - 1, s, x - HALO] + product
                if h < halves - 1:
                    sums[n - 1, s, x - HALO] = total
                else:
                    moments_ref[n - 1, s, pl.ds(x - HALO, 1), :] = (
                        jnp.sum(total, axis=0, keepdims=True) * (1.0 / vectors))
                if n == 1:
                    extra = ((0, product), (4, start * start))
                elif n == 2:
                    extra = (
                        (1, product),
                        (2, now_r * results[0] + now_i * results[1]),
                        (3, results[0] * results[0] + results[1] * results[1]),
                    )
                else:
                    extra = ()
                for slot, value in extra:
                    total = traces[h, slot]
                    for k in range(blocks):
                        total = total + value[:, k * BLOCK : (k + 1) * BLOCK]
                    traces[h, slot] = total

            row(where(t), measured)
            return carry

        lax.fori_loop(0, count, middle if measure else plain, 0, unroll=True)

    def inside(n, h):
        term(n, h, wide - 2 * n, lambda t: HALO + n + t, True)

    def border(n, h):
        term(n, h, 2 * n, lambda t: HALO + t + (wide - 2 * n) * (t // n), True)

    def halo_edges():
        return {a: edge_side[0 if a == -1 else 1].astype(F32) for a in (1, -1)}

    def near_stage(h):
        for a in (1, -1):
            if h == 0:
                halos[h]["edge", a].wait()
            halos[h]["near", a].wait_recv()
            if h < halves - 1:
                halos[h]["near", a].wait_send()
        edges = halo_edges()
        begin(h, HALO - NEAR, HALO, (edges[1], wide - NEAR))
        begin(h, HALO + wide, HALO + wide + NEAR, (edges[-1], 0))
        term(1, h, 2, lambda t: HALO - 1 + t * (wide + 1), False)
        border(1, h)
        border(2, h)

    def far_stage(h):
        for a in (1, -1):
            halos[h]["far", a].wait()
        edges = halo_edges()
        begin(h, 0, HALO - NEAR, (edges[1], wide - HALO))
        begin(h, HALO + wide + NEAR, 2 * HALO + wide, (edges[-1], NEAR))
        term(1, h, 4, lambda t: 1 + t + (t // 2) * (wide + 2), False)
        term(2, h, 4, lambda t: 2 + t + (t // 2) * wide, False)
        term(3, h, 2, lambda t: 3 + t * (wide + 1), False)
        border(3, h)
        term(TERMS, h, wide, lambda t: HALO + t, True)

    small = lax.broadcasted_iota(jnp.int32, (GROUP, BLOCK), 1)
    slot_of = lax.broadcasted_iota(jnp.int32, (GROUP, BLOCK), 0)

    def gather_traces(h):
        out = jnp.zeros((GROUP, BLOCK), F32)
        for n in range(TERMS):
            value = traces[h, n]
            if n == 2:
                value = 2.0 * value - traces[h, 0]
            if n == 3:
                value = 2.0 * value - traces[h, 4]
            total = jnp.sum(value, axis=1, keepdims=True)
            out = jnp.where(small == slot_of + (n * vectors + h * GROUP), total, out)
        return jnp.sum(out, axis=0, keepdims=True)

    trace_row = jnp.zeros((1, BLOCK), F32)
    for h in range(halves):
        arrive(h)
        for n in range(1, TERMS):
            inside(n, h)
    far_sites()
    for a in (1, -1):
        halos[halves - 1]["near", a].wait_send()
    for h in range(halves):
        send_rows(h, "far")
    for h in range(halves):
        near_stage(h)
        trace_row = trace_row + gather_traces(h)
    part[...] = trace_row
    me = gx * ny + gy
    parts[me] = trace_row
    sent = []
    for i in range(1, many):
        move = copy(part, parts.at[me], sum_send.at[i], sum_recv.at[i], at(i // ny, i % ny))
        move.start()
        sent.append(move)
    for h in range(halves):
        far_stage(h)
    for move in sent:
        move.wait()
    total = parts[0]
    for p in range(1, many):
        total = total + parts[p]
    sites_total = 2 * wide * nx * long * ny
    total = total * (1.0 / sites_total)
    for n in range(TERMS):
        turned_row = pltpu.roll(total, BLOCK - n * vectors, axis=1) if n else total
        trace_ref[n : n + 1, :] = turned_row[:, :vectors]


def local(nx, ny, stored_vectors, disorder, vacancy, plan):
    vectors, wide, long = stored_vectors.shape[1:]
    tall, extent = wide + 2 * HALO, long + BLOCK
    halves, blocks, pair = vectors // GROUP, long // BLOCK, 2 * GROUP
    dma = pltpu.SemaphoreType.DMA
    many = nx * ny
    field = pltpu.VMEM((halves, 2, tall, GROUP, extent), F32)
    return pl.pallas_call(
        functools.partial(program, nx, ny),
        out_shape=(
            pltpu.VMEM((TERMS, 2, wide, long), F32),
            pltpu.VMEM((TERMS, vectors), F32),
        ),
        in_specs=[pl.BlockSpec(memory_space=pl.ANY)] * 4,
        out_specs=(pl.BlockSpec(memory_space=pltpu.VMEM),) * 2,
        scratch_shapes=[
            pltpu.SMEM(plan.shape, jnp.int32),
            pltpu.VMEM(stored_vectors.shape, BF16),
            pltpu.VMEM(disorder.shape, F32),
            pltpu.VMEM(vacancy.shape, jnp.int32),
            pltpu.VMEM((halves, blocks, wide, pair, BLOCK), BF16),
            pltpu.VMEM((blocks, pair, BLOCK), F32),
            pltpu.VMEM((halves, ny, wide, pair, BLOCK), BF16),
            pltpu.VMEM((ny, pair, BLOCK), BF16),
            pltpu.VMEM((ny, pair, BLOCK), BF16),
            pltpu.VMEM((halves, tall, pair, long), BF16),
            pltpu.VMEM((pair, BLOCK), BF16),
            pltpu.VMEM((2, pair, BLOCK), BF16),
            pltpu.VMEM((2, 2, 2 * HALO, long), F32),
            pltpu.VMEM((2, 2, 2 * HALO, long), F32),
            pltpu.VMEM((2, 1, BLOCK), F32),
            pltpu.VMEM((2, 2, 1, BLOCK), F32),
            pltpu.VMEM((2, 1, BLOCK), F32),
            pltpu.VMEM((2, 2, 1, BLOCK), F32),
        ]
        + [pltpu.VMEM((2, tall, extent), F32)] * 3
        + [field] * 7
        + [
            pltpu.VMEM((TERMS, 2, wide, GROUP, long), F32),
            pltpu.VMEM((halves, TERMS + 1, GROUP, BLOCK), F32),
            pltpu.VMEM((1, BLOCK), F32),
            pltpu.VMEM((many, 1, BLOCK), F32),
            dma((4,)),
            dma((halves + 1, ny)), dma((halves + 1, ny)),
            dma((halves, 2, 3)), dma((halves, 2, 3)),
            dma((6,)), dma((6,)),
            dma((many,)), dma((many,)),
            pltpu.SemaphoreType.REGULAR((nx - 2, 2)),
        ]
        + [pltpu.VMEM((ny, wide, pair, BLOCK), BF16)] * halves,
        compiler_params=pltpu.CompilerParams(collective_id=0, has_side_effects=True),
        name="chebyshev",
    )(plan, stored_vectors, disorder, vacancy)


def solution(mesh):
    placed = (P(None, None, "gx", "gy"), P(None, "gx", "gy"), P(None, "gx", "gy"), P())
    return jax.shard_map(
        functools.partial(local, mesh.shape["gx"], mesh.shape["gy"]),
        mesh=mesh,
        in_specs=placed,
        out_specs=(P(None, None, "gx", "gy"), P()),
        check_vma=False,
    )
```

```python
import functools

import jax
import jax.numpy as jnp
from jax import lax
from jax.experimental import pallas as pl
from jax.experimental.pallas import tpu as pltpu
from jax.sharding import PartitionSpec as P

BLOCK = 128
TERMS = 4
HOP_NEXT = 0.3
TWIST_COS = 0.4535961214255773
TWIST_SIN = 0.8912073600614354
SPREAD = 6.5
HALO = TERMS
NEAR = 2
GROUP = 8
MESH = pl.DeviceIdType.MESH
F32 = jnp.float32
BF16 = jnp.bfloat16

def rows_from(a, wide):
    if a == 0:
        return slice(HALO, HALO + wide)
    return slice(0, HALO) if a == 1 else slice(HALO + wide, 2 * HALO + wide)


def rows_to(a, wide):
    if a == 0:
        return slice(0, wide)
    return slice(wide - HALO, wide) if a == 1 else slice(0, HALO)


def program(
    nx, ny,
    plan_any, stored_any, disorder_any, vacancy_any,
    moments_ref, trace_ref,
    plan_ref, stored_ref, disorder_ref, vacancy_ref,
    turned, strips, send, edge_send, edge_recv, lattice, edge_own, edge_side,
    site_send_x, site_x, site_edge, site_y, site_both, site_z, keep_ref, onsite, factor,
    real0, real1, real2, real3, imag1, imag2, imag3, sums, traces, part, parts,
    load_sem, a2a_send, a2a_recv, halo_send, halo_recv, site_send, site_recv, sum_send, sum_recv, token,
    *landing,
):
    gx, gy = lax.axis_index("gx"), lax.axis_index("gy")
    wide, long = disorder_ref.shape[1], disorder_ref.shape[2]
    halves = lattice.shape[0]
    vectors = halves * GROUP
    recv = landing
    extent = long + BLOCK
    blocks = long // BLOCK
    many = nx * ny
    cos, sin = HOP_NEXT * TWIST_COS, HOP_NEXT * TWIST_SIN

    def at(a, b):
        return (lax.rem(gx + a + nx, nx), lax.rem(gy + b + ny, ny))

    cores = 2 if ny % 2 == 0 else 1
    cols = 2 if (ny // cores) % 2 == 0 else 1
    lines = ny // (cores * cols)
    steps = [(r, c, u) for r in range(lines) for c in range(cols) for u in range(cores)]
    steps.sort(key=lambda step: -((step[0] != 0) + (step[1] != 0)))
    steps = [(0, 0, 0)] + [step for step in steps if step != (0, 0, 0)]

    def peer(i):
        r, c, u = steps[i]
        line = lax.rem(gy // (cores * cols) + r, lines)
        col = lax.rem(lax.rem(gy // cores, cols) + c, cols)
        return (line * cols + col) * cores + lax.rem(lax.rem(gy, cores) + u, cores)

    def copy(source, target, out_sem, in_sem, device):
        return pltpu.make_async_remote_copy(
            src_ref=source, dst_ref=target, send_sem=out_sem, recv_sem=in_sem,
            device_id=device, device_id_type=MESH,
        )

    def drain(span, out_sem, in_sem):
        return copy(span, span, out_sem, in_sem, at(0, 0))

    loads = []
    for t, (source, target) in enumerate((
        (stored_any, stored_ref), (plan_any, plan_ref),
        (disorder_any, disorder_ref), (vacancy_any, vacancy_ref),
    )):
        loads.append(pltpu.make_async_copy(source, target, load_sem.at[t]))
        loads[-1].start()
    barrier = pltpu.get_barrier_semaphore()
    linked = {-1: gx > 0, 1: gx < nx - 1}

    def greet(sem, a, b):
        pl.semaphore_signal(sem, inc=1, device_id=at(a, b), device_id_type=MESH)

    for b in range(1, ny):
        greet(barrier, 0, b)
    for a in (-1, 1):
        pl.when(linked[a])(functools.partial(greet, barrier, a, 0))
    entered = ny - 1 + linked[-1].astype(jnp.int32) + linked[1].astype(jnp.int32)

    def pass_on(step):
        for side, a in enumerate((-1, 1)):
            pl.when(linked[a])(functools.partial(greet, token.at[step, 1 - side], a, 0))

    def hear(step):
        for side, a in enumerate((-1, 1)):
            pl.when(linked[a])(functools.partial(pl.semaphore_wait, token.at[step, side], 1))

    traces[...] = jnp.zeros_like(traces)
    for load in loads:
        load.wait()

    lane = lax.broadcasted_iota(jnp.int32, (2 * GROUP, BLOCK), 1)
    place = ((lane + HALO) & (BLOCK - 1)) // (2 * HALO)
    is_last = (lane & HALO) != 0

    def turn(h):
        for k in range(blocks):
            piece = stored_ref[:, h * GROUP : (h + 1) * GROUP, :, k * BLOCK : (k + 1) * BLOCK]
            piece = piece.astype(F32).reshape(2 * GROUP, wide, BLOCK)
            piece = jnp.transpose(piece, (1, 0, 2))
            turned[h, k] = piece.astype(BF16)
            strip = strips[k] if h else piece[0]
            for x in range(0 if h else 1, wide):
                spot = h * wide + x
                moved = pltpu.roll(piece[x], 2 * HALO * spot, axis=1)
                strip = jnp.where(place == spot, moved, strip)
            strips[k] = strip

    def mine(index):
        return plan_ref[lax.rem(index + ny * blocks, ny * blocks)] - gy * blocks

    def inside_mine(offset):
        return (offset >= 0) & (offset < blocks)

    picks = []
    for i in range(ny):
        target = peer(i)
        pick = 0
        for j in range(blocks):
            offset = mine(target * blocks + j)
            pick = jnp.where(inside_mine(offset), offset, pick)
        left, right = mine(target * blocks - 1), mine(target * blocks + blocks)
        left = jnp.where(inside_mine(left), left, 0)
        right = jnp.where(inside_mine(right), right, 0)
        picks.append((pick, left, right))

    def fill(h):
        for i in range(1, ny):
            send[h, i] = turned[h, picks[i][0]]
        recv[h][gy] = turned[h, picks[0][0]]

    def fill_edges():
        def edge(i):
            return jnp.where(is_last, strips[picks[i][1]], strips[picks[i][2]]).astype(BF16)
        for i in range(1, ny):
            edge_send[i] = edge(i)
        edge_recv[gy] = edge(0)

    def start_blocks(h):
        for i in range(1, ny):
            copy(send.at[h, i], recv[h].at[gy], a2a_send.at[h], a2a_recv.at[h],
                 (gx, peer(i))).start()

    def start_edges():
        for i in range(1, ny):
            copy(edge_send.at[i], edge_recv.at[gy], a2a_send.at[halves], a2a_recv.at[halves],
                 (gx, peer(i))).start()

    block_drains = [
        drain(recv[h].at[0 : ny - 1], a2a_send.at[h], a2a_recv.at[h]) for h in range(halves)
    ]
    edge_drain = drain(edge_recv.at[0 : ny - 1], a2a_send.at[halves], a2a_recv.at[halves])

    turn(0)
    fill(0)
    site_lane = lax.broadcasted_iota(jnp.int32, (2, wide, BLOCK), 2)
    site_row = lax.broadcasted_iota(jnp.int32, (2, wide, BLOCK), 1)
    span = 4 * HALO
    low = site_lane < BLOCK // 2
    keep_own = vacancy_ref[...].astype(F32)
    ends = []
    for own in (disorder_ref[...], keep_own):
        ends.append(jnp.where(low, own[:, :, 0:BLOCK], own[:, :, long - BLOCK : long]))
    keep_end = jnp.where(low, pltpu.roll(ends[1], HALO, axis=2),
                         pltpu.roll(ends[1], BLOCK - HALO, axis=2))
    packed = jnp.where(((site_lane + HALO) & (BLOCK - 1)) < 2 * HALO, ends[0], keep_end)
    packed = pltpu.roll(packed, 0, axis=2, stride=span, stride_axis=1)
    packed = jnp.where(((site_lane + span // 2) & (BLOCK - 1)) // span == site_row, packed, 0.0)
    site_edge[...] = jnp.sum(packed, axis=1, keepdims=True)
    for a in (-1, 1):
        kept = rows_to(a, wide)
        rows = (disorder_ref[:, kept, :], keep_own[:, kept, :])
        site_send_x[0 if a == -1 else 1] = jnp.concatenate(rows, axis=1)
    sites = {}

    def site(name, source, target, w, device, when=None):
        sites[name] = copy(source, target, site_send.at[w], site_recv.at[w], device)
        if when is None:
            sites[name].start()
        else:
            pl.when(when)(sites[name].start)

    x_drain = drain(site_x, site_send.at[0], site_recv.at[0])
    y_drain = drain(site_y, site_send.at[1], site_recv.at[1])
    z_drain = drain(site_z, site_send.at[2], site_recv.at[2])

    pl.semaphore_wait(barrier, entered)
    pass_on(0)
    for side, a in enumerate((-1, 1)):
        site(("x", a), site_send_x.at[side], site_x.at[side], 0, at(a, 0), linked[a])
        site(("y", a), site_edge, site_y.at[side], 1, at(0, a))
    start_blocks(0)

    for h in range(1, halves):
        turn(h)
    fill_edges()
    start_edges()
    def token_round(step):
        hear(step)
        if step < nx - 3:
            pass_on(step + 1)

    for step in range(nx - 3):
        token_round(step)
    for h in range(1, halves):
        fill(h)
        block_drains[h - 1].wait_send()
        start_blocks(h)
    token_round(nx - 3)
    for a in (-1, 1):
        pl.when(~linked[a])(sites["x", a].start)

    short = lax.broadcasted_iota(jnp.int32, (2, 1, BLOCK), 2)

    def site_ends(a, both):
        rows, kept = rows_from(a, wide), rows_to(a, wide)
        for x in range(rows.start, rows.stop):
            shift = 2 * BLOCK - span * (x - rows.start + kept.start)
            energy = pltpu.roll(both, shift % BLOCK, axis=2)
            present = jnp.where(short < BLOCK // 2,
                                pltpu.roll(both, (shift - HALO) % BLOCK, axis=2),
                                pltpu.roll(both, (shift + HALO) % BLOCK, axis=2))
            scale = present * (1.0 / SPREAD)
            keep_ref[:, x : x + 1, long:] = present
            factor[:, x : x + 1, long:] = scale
            onsite[:, x : x + 1, long:] = energy * scale

    def site_rows(a, energy, present):
        rows = rows_from(a, wide)
        scale = present * (1.0 / SPREAD)
        keep_ref[:, rows, 0:long] = present
        factor[:, rows, 0:long] = scale
        onsite[:, rows, 0:long] = energy * scale

    site_rows(0, disorder_ref[...], keep_own)
    y_drain.wait()
    site_both[...] = jnp.where((short & (span // 2)) == 0, site_y[0], site_y[1])
    for side, a in enumerate((-1, 1)):
        site(("z", a), site_both, site_z.at[side], 2, at(a, 0))
    site_ends(0, site_both[...])

    def far_sites():
        x_drain.wait()
        z_drain.wait()
        for side, a in enumerate((-1, 1)):
            site_rows(a, site_x[side, :, 0:HALO], site_x[side, :, HALO:])
            site_ends(a, site_z[side])

    def begin(h, first, last, edges):
        for x in range(first, last):
            rows = lattice[h, x].astype(F32)
            shift = (-2 * HALO * (h * wide + edges[1] + x - first)) % BLOCK
            edge = pltpu.roll(edges[0], shift, axis=1) if shift else edges[0]
            for s in range(2):
                mask = keep_ref[s, x : x + 1, :]
                own = slice(s * GROUP, (s + 1) * GROUP)
                real0[h, s, x, :, 0:long] = rows[own] * mask[:, 0:long]
                real0[h, s, x, :, long:] = edge[own] * mask[:, long:]

    near_drains = [
        drain(lattice.at[h, 0 : 2 * NEAR], halo_send.at[h, 0], halo_recv.at[h, 0])
        for h in range(halves)
    ]
    far_drains = [
        drain(lattice.at[h, 0 : 2 * NEAR], halo_send.at[h, 1], halo_recv.at[h, 1])
        for h in range(halves)
    ]
    side_drain = drain(edge_side, halo_send.at[0, 2], halo_recv.at[0, 2])

    def halo(h, a, source, target, slot):
        copy(source, target, halo_send.at[h, slot], halo_recv.at[h, slot], at(a, 0)).start()

    def own_edge():
        left = plan_ref[lax.rem(gy * blocks - 1 + ny * blocks, ny * blocks)] // blocks
        right = plan_ref[lax.rem(gy * blocks + blocks, ny * blocks)] // blocks
        return jnp.where(is_last, edge_recv[left].astype(F32), edge_recv[right].astype(F32))

    def send_rows(h, name):
        for a in (1, -1):
            last = (a == 1) == (name == "near")
            cut = slice(HALO - NEAR, HALO) if last else slice(0, NEAR)
            rows_out, rows_in = rows_to(a, wide).start + HALO, rows_from(a, wide).start
            source = lattice.at[h, rows_out + cut.start : rows_out + cut.stop]
            target = lattice.at[h, rows_in + cut.start : rows_in + cut.stop]
            halo(h, a, source, target, 0 if name == "near" else 1)

    def arrive(h):
        block_drains[h].wait_recv()
        if h == halves - 1:
            block_drains[h].wait_send()
        for k in range(blocks):
            source = plan_ref[gy * blocks + k] // blocks
            lattice[h, HALO : HALO + wide, :, k * BLOCK : (k + 1) * BLOCK] = recv[h][source]
        send_rows(h, "near")
        if h == 0:
            edge_drain.wait()
            edge_own[...] = own_edge().astype(BF16)
            for a in (1, -1):
                halo(0, a, edge_own, edge_side.at[0 if a == -1 else 1], 2)
        begin(h, HALO, HALO + wide, (own_edge(), 0))

    def back(value):
        return pltpu.roll(value, 1, axis=1)

    def ahead(value):
        return pltpu.roll(value, extent - 1, axis=1)

    def bond(r, i, first, second, chiral, want_imag):
        turn = chiral * sin
        out_real = cos * (r[first] + r[second])
        if i is not None:
            out_real = out_real - turn * (i[first] - i[second])
        out_imag = None
        if want_imag:
            out_imag = turn * (r[first] - r[second])
            if i is not None:
                out_imag = out_imag + cos * (i[first] + i[second])
        return out_real, out_imag

    reals_of = (real0, real1, real2, real3)
    imags_of = (None, imag1, imag2, imag3)

    def term(n, h, count, where, measure):
        if count <= 0:
            return
        cur_r, cur_i = reals_of[n - 1], imags_of[n - 1]
        complex_in, want_imag, keep_new = n > 1, n < TERMS, n < TERMS

        def row(x, measured):
            reals = [[cur_r[h, s, x + d] for d in (-1, 0, 1)] for s in range(2)]
            imags = [None, None]
            if complex_in:
                imags = [[cur_i[h, s, x + d] for d in (-1, 0, 1)] for s in range(2)]
            for s, chiral in ((0, 1.0), (1, -1.0)):
                r, i = reals[s], imags[s]
                other_r, other_i = reals[1 - s], imags[1 - s]
                here = bond(r, i, 2, 0, chiral, want_imag)
                behind = bond(r, i, 1, 2, chiral, want_imag)
                front = bond(r, i, 0, 1, chiral, want_imag)
                level = onsite[s, pl.ds(x, 1), :]
                scale = factor[s, pl.ds(x, 1), :]
                if n > 1:
                    level, scale = 2.0 * level, 2.0 * scale
                away = 0 if s == 0 else 2
                results = []
                for part_of in range(2 if want_imag else 1):
                    own, other = (r, other_r) if part_of == 0 else (i, other_i)
                    hop, prior, later = here[part_of], behind[part_of], front[part_of]
                    if other is not None:
                        hop = hop - (other[1] + other[away])
                        if s == 0:
                            prior = prior - other[1]
                        else:
                            later = later - other[1]
                    result = (hop + (back(prior) + ahead(later))) * scale
                    if own is not None:
                        result = result + level * own[1]
                    fields = reals_of if part_of == 0 else imags_of
                    if n > 1 and fields[n - 2] is not None:
                        result = result - fields[n - 2][h, s, x]
                    if keep_new:
                        fields[n][h, s, x] = result
                    results.append(result[:, :long])
                if measured is not None:
                    measured(s, x, real0[h, s, x, :, 0:long], results,
                             r[1][:, :long], None if i is None else i[1][:, :long])

        def plain(t, carry):
            row(where(t), None)
            return carry

        def middle(t, carry):
            def measured(s, x, start, results, now_r, now_i):
                product = start * results[0]
                total = product
                if h > 0:
                    total = sums[n - 1, s, x - HALO] + product
                if h < halves - 1:
                    sums[n - 1, s, x - HALO] = total
                else:
                    moments_ref[n - 1, s, pl.ds(x - HALO, 1), :] = (
                        jnp.sum(total, axis=0, keepdims=True) * (1.0 / vectors))
                if n == 1:
                    extra = ((0, product), (4, start * start))
                elif n == 2:
                    extra = (
                        (1, product),
                        (2, now_r * results[0] + now_i * results[1]),
                        (3, results[0] * results[0] + results[1] * results[1]),
                    )
                else:
                    extra = ()
                for slot, value in extra:
                    total = traces[h, slot]
                    for k in range(blocks):
                        total = total + value[:, k * BLOCK : (k + 1) * BLOCK]
                    traces[h, slot] = total

            row(where(t), measured)
            return carry

        lax.fori_loop(0, count, middle if measure else plain, 0, unroll=True)

    def inside(n, h):
        term(n, h, wide - 2 * n, lambda t: HALO + n + t, True)

    def border(n, h):
        term(n, h, 2 * n, lambda t: HALO + t + (wide - 2 * n) * (t // n), True)

    def halo_edges():
        return {a: edge_side[0 if a == -1 else 1].astype(F32) for a in (1, -1)}

    def near_stage(h):
        if h == 0:
            side_drain.wait()
        near_drains[h].wait_recv()
        if h < halves - 1:
            near_drains[h].wait_send()
        edges = halo_edges()
        begin(h, HALO - NEAR, HALO, (edges[1], wide - NEAR))
        begin(h, HALO + wide, HALO + wide + NEAR, (edges[-1], 0))
        term(1, h, 2, lambda t: HALO - 1 + t * (wide + 1), False)
        border(1, h)
        border(2, h)

    def far_stage(h):
        far_drains[h].wait()
        edges = halo_edges()
        begin(h, 0, HALO - NEAR, (edges[1], wide - HALO))
        begin(h, HALO + wide + NEAR, 2 * HALO + wide, (edges[-1], NEAR))
        term(1, h, 4, lambda t: 1 + t + (t // 2) * (wide + 2), False)
        term(2, h, 4, lambda t: 2 + t + (t // 2) * wide, False)
        term(3, h, 2, lambda t: 3 + t * (wide + 1), False)
        border(3, h)
        term(TERMS, h, wide, lambda t: HALO + t, True)

    small = lax.broadcasted_iota(jnp.int32, (GROUP, BLOCK), 1)
    slot_of = lax.broadcasted_iota(jnp.int32, (GROUP, BLOCK), 0)

    def gather_traces(h):
        out = jnp.zeros((GROUP, BLOCK), F32)
        for n in range(TERMS):
            value = traces[h, n]
            if n == 2:
                value = 2.0 * value - traces[h, 0]
            if n == 3:
                value = 2.0 * value - traces[h, 4]
            total = jnp.sum(value, axis=1, keepdims=True)
            out = jnp.where(small == slot_of + (n * vectors + h * GROUP), total, out)
        return jnp.sum(out, axis=0, keepdims=True)

    trace_row = jnp.zeros((1, BLOCK), F32)
    for h in range(halves):
        arrive(h)
        for n in range(1, TERMS):
            inside(n, h)
    far_sites()
    near_drains[halves - 1].wait_send()
    for h in range(halves):
        send_rows(h, "far")
    for h in range(halves):
        near_stage(h)
        trace_row = trace_row + gather_traces(h)
    part[...] = trace_row
    me = gx * ny + gy
    parts[me] = trace_row
    for i in range(1, many):
        copy(part, parts.at[me], sum_send.at[0], sum_recv.at[0], at(i // ny, i % ny)).start()
    for h in range(halves):
        far_stage(h)
    drain(parts.at[0 : many - 1], sum_send.at[0], sum_recv.at[0]).wait()
    total = parts[0]
    for p in range(1, many):
        total = total + parts[p]
    sites_total = 2 * wide * nx * long * ny
    total = total * (1.0 / sites_total)
    for n in range(TERMS):
        turned_row = pltpu.roll(total, BLOCK - n * vectors, axis=1) if n else total
        trace_ref[n : n + 1, :] = turned_row[:, :vectors]


def store(moments_ref, trace_ref, moments_any, trace_any, sems):
    copies = [
        pltpu.make_async_copy(trace_ref, trace_any, sems.at[0]),
        pltpu.make_async_copy(moments_ref, moments_any, sems.at[1]),
    ]
    for move in copies:
        move.start()
    for move in copies:
        move.wait()


def local(nx, ny, stored_vectors, disorder, vacancy, plan):
    vectors, wide, long = stored_vectors.shape[1:]
    tall, extent = wide + 2 * HALO, long + BLOCK
    halves, blocks, pair = vectors // GROUP, long // BLOCK, 2 * GROUP
    dma = pltpu.SemaphoreType.DMA
    many = nx * ny
    field = pltpu.VMEM((halves, 2, tall, GROUP, extent), F32)
    moments, trace = pl.pallas_call(
        functools.partial(program, nx, ny),
        out_shape=(
            pltpu.VMEM((TERMS, 2, wide, long), F32),
            pltpu.VMEM((TERMS, vectors), F32),
        ),
        in_specs=[pl.BlockSpec(memory_space=pl.ANY)] * 4,
        out_specs=(pl.BlockSpec(memory_space=pltpu.VMEM),) * 2,
        scratch_shapes=[
            pltpu.SMEM(plan.shape, jnp.int32),
            pltpu.VMEM(stored_vectors.shape, BF16),
            pltpu.VMEM(disorder.shape, F32),
            pltpu.VMEM(vacancy.shape, jnp.int32),
            pltpu.VMEM((halves, blocks, wide, pair, BLOCK), BF16),
            pltpu.VMEM((blocks, pair, BLOCK), F32),
            pltpu.VMEM((halves, ny, wide, pair, BLOCK), BF16),
            pltpu.VMEM((ny, pair, BLOCK), BF16),
            pltpu.VMEM((ny, pair, BLOCK), BF16),
            pltpu.VMEM((halves, tall, pair, long), BF16),
            pltpu.VMEM((pair, BLOCK), BF16),
            pltpu.VMEM((2, pair, BLOCK), BF16),
            pltpu.VMEM((2, 2, 2 * HALO, long), F32),
            pltpu.VMEM((2, 2, 2 * HALO, long), F32),
            pltpu.VMEM((2, 1, BLOCK), F32),
            pltpu.VMEM((2, 2, 1, BLOCK), F32),
            pltpu.VMEM((2, 1, BLOCK), F32),
            pltpu.VMEM((2, 2, 1, BLOCK), F32),
        ]
        + [pltpu.VMEM((2, tall, extent), F32)] * 3
        + [field] * 7
        + [
            pltpu.VMEM((TERMS, 2, wide, GROUP, long), F32),
            pltpu.VMEM((halves, TERMS + 1, GROUP, BLOCK), F32),
            pltpu.VMEM((1, BLOCK), F32),
            pltpu.VMEM((many, 1, BLOCK), F32),
            dma((4,)),
            dma((halves + 1,)), dma((halves + 1,)),
            dma((halves, 3)), dma((halves, 3)),
            dma((3,)), dma((3,)),
            dma((1,)), dma((1,)),
            pltpu.SemaphoreType.REGULAR((nx - 2, 2)),
        ]
        + [pltpu.VMEM((ny, wide, pair, BLOCK), BF16)] * halves,
        compiler_params=pltpu.CompilerParams(collective_id=0, has_side_effects=True),
        name="chebyshev",
    )(plan, stored_vectors, disorder, vacancy)
    moments = pltpu.with_memory_space_constraint(moments, pltpu.VMEM)
    trace = pltpu.with_memory_space_constraint(trace, pltpu.VMEM)
    return pl.pallas_call(
        store,
        out_shape=(
            jax.ShapeDtypeStruct(moments.shape, F32),
            jax.ShapeDtypeStruct(trace.shape, F32),
        ),
        in_specs=[pl.BlockSpec(memory_space=pltpu.VMEM)] * 2,
        out_specs=(pl.BlockSpec(memory_space=pl.ANY),) * 2,
        scratch_shapes=[dma((2,))],
        name="store",
    )(moments, trace)


def solution(mesh):
    placed = (P(None, None, "gx", "gy"), P(None, "gx", "gy"), P(None, "gx", "gy"), P())
    return jax.shard_map(
        functools.partial(local, mesh.shape["gx"], mesh.shape["gy"]),
        mesh=mesh,
        in_specs=placed,
        out_specs=(P(None, None, "gx", "gy"), P()),
        check_vma=False,
    )
```

```python
import functools

import jax
import jax.numpy as jnp
from jax import lax
from jax.experimental import pallas as pl
from jax.experimental.pallas import tpu as pltpu
from jax.sharding import PartitionSpec as P

BLOCK = 128
TERMS = 4
HOP_NEXT = 0.3
TWIST_COS = 0.4535961214255773
TWIST_SIN = 0.8912073600614354
SPREAD = 6.5
HALO = TERMS
NEAR = 2
GROUP = 8
MESH = pl.DeviceIdType.MESH
F32 = jnp.float32
BF16 = jnp.bfloat16

def rows_from(a, wide):
    if a == 0:
        return slice(HALO, HALO + wide)
    return slice(0, HALO) if a == 1 else slice(HALO + wide, 2 * HALO + wide)


def rows_to(a, wide):
    if a == 0:
        return slice(0, wide)
    return slice(wide - HALO, wide) if a == 1 else slice(0, HALO)


def program(
    nx, ny,
    plan_any, stored_any, disorder_any, vacancy_any,
    moments_ref, trace_ref,
    plan_ref, stored_ref, disorder_ref, vacancy_ref,
    turned, strips, send, edge_send, edge_recv, lattice, edge_own, edge_side,
    site_send_x, site_x, site_edge, site_y, site_both, site_z, keep_ref, onsite, factor,
    real0, real1, real2, real3, imag1, imag2, imag3, sums, traces, part, parts,
    load_sem, a2a_send, a2a_recv, halo_send, halo_recv, site_send, site_recv, sum_send, sum_recv, direct_send, direct_recv, token,
    *landing,
):
    gx, gy = lax.axis_index("gx"), lax.axis_index("gy")
    wide, long = disorder_ref.shape[1], disorder_ref.shape[2]
    halves = lattice.shape[0]
    vectors = halves * GROUP
    recv, near_in = landing[:halves], landing[halves]
    extent = long + BLOCK
    blocks = long // BLOCK
    many = nx * ny
    cos, sin = HOP_NEXT * TWIST_COS, HOP_NEXT * TWIST_SIN

    def at(a, b):
        return (lax.rem(gx + a + nx, nx), lax.rem(gy + b + ny, ny))

    cores = 2 if ny % 2 == 0 else 1
    cols = 2 if (ny // cores) % 2 == 0 else 1
    lines = ny // (cores * cols)
    steps = [(r, c, u) for r in range(lines) for c in range(cols) for u in range(cores)]
    steps.sort(key=lambda step: -((step[0] != 0) + (step[1] != 0)))
    steps = [(0, 0, 0)] + [step for step in steps if step != (0, 0, 0)]

    def peer(i):
        r, c, u = steps[i]
        line = lax.rem(gy // (cores * cols) + r, lines)
        col = lax.rem(lax.rem(gy // cores, cols) + c, cols)
        return (line * cols + col) * cores + lax.rem(lax.rem(gy, cores) + u, cores)

    def copy(source, target, out_sem, in_sem, device):
        return pltpu.make_async_remote_copy(
            src_ref=source, dst_ref=target, send_sem=out_sem, recv_sem=in_sem,
            device_id=device, device_id_type=MESH,
        )

    def drain(span, out_sem, in_sem):
        return copy(span, span, out_sem, in_sem, at(0, 0))

    loads = []
    for t, (source, target) in enumerate((
        (stored_any, stored_ref), (plan_any, plan_ref),
        (disorder_any, disorder_ref), (vacancy_any, vacancy_ref),
    )):
        loads.append(pltpu.make_async_copy(source, target, load_sem.at[t]))
        loads[-1].start()
    barrier = pltpu.get_barrier_semaphore()
    linked = {-1: gx > 0, 1: gx < nx - 1}

    def greet(sem, a, b):
        pl.semaphore_signal(sem, inc=1, device_id=at(a, b), device_id_type=MESH)

    for b in range(1, ny):
        greet(barrier, 0, b)
    for a in (-1, 1):
        pl.when(linked[a])(functools.partial(greet, barrier, a, 0))
    entered = ny - 1 + linked[-1].astype(jnp.int32) + linked[1].astype(jnp.int32)

    def pass_on(step):
        for side, a in enumerate((-1, 1)):
            pl.when(linked[a])(functools.partial(greet, token.at[step, 1 - side], a, 0))

    def hear(step):
        for side, a in enumerate((-1, 1)):
            pl.when(linked[a])(functools.partial(pl.semaphore_wait, token.at[step, side], 1))

    traces[...] = jnp.zeros_like(traces)
    for load in loads:
        load.wait()

    lane = lax.broadcasted_iota(jnp.int32, (2 * GROUP, BLOCK), 1)
    place = ((lane + HALO) & (BLOCK - 1)) // (2 * HALO)
    is_last = (lane & HALO) != 0

    def turn(h):
        for k in range(blocks):
            piece = stored_ref[:, h * GROUP : (h + 1) * GROUP, :, k * BLOCK : (k + 1) * BLOCK]
            piece = piece.astype(F32).reshape(2 * GROUP, wide, BLOCK)
            piece = jnp.transpose(piece, (1, 0, 2))
            turned[h, k] = piece.astype(BF16)
            strip = strips[k] if h else piece[0]
            for x in range(0 if h else 1, wide):
                spot = h * wide + x
                moved = pltpu.roll(piece[x], 2 * HALO * spot, axis=1)
                strip = jnp.where(place == spot, moved, strip)
            strips[k] = strip

    def mine(index):
        return plan_ref[lax.rem(index + ny * blocks, ny * blocks)] - gy * blocks

    def inside_mine(offset):
        return (offset >= 0) & (offset < blocks)

    picks = []
    for i in range(ny):
        target = peer(i)
        pick = 0
        for j in range(blocks):
            offset = mine(target * blocks + j)
            pick = jnp.where(inside_mine(offset), offset, pick)
        left, right = mine(target * blocks - 1), mine(target * blocks + blocks)
        left = jnp.where(inside_mine(left), left, 0)
        right = jnp.where(inside_mine(right), right, 0)
        picks.append((pick, left, right))

    final = halves - 1

    def fill(h):
        for i in range(0 if h == final else 1, ny):
            send[h, i] = turned[h, picks[i][0]]
        recv[h][gy] = turned[h, picks[0][0]]

    def fill_edges():
        def edge(i):
            return jnp.where(is_last, strips[picks[i][1]], strips[picks[i][2]]).astype(BF16)
        for i in range(1, ny):
            edge_send[i] = edge(i)
        edge_recv[gy] = edge(0)

    def start_blocks(h):
        for i in range(1, ny):
            copy(send.at[h, i], recv[h].at[gy], a2a_send.at[h], a2a_recv.at[h],
                 (gx, peer(i))).start()

    def start_direct(a):
        rows = slice(wide - NEAR, wide) if a == 1 else slice(0, NEAR)
        for i in range(ny):
            copy(send.at[final, i, rows], near_in.at[gy], direct_send.at[0], direct_recv.at[0],
                 (lax.rem(gx + a + nx, nx), peer(i))).start()

    def start_edges():
        for i in range(1, ny):
            copy(edge_send.at[i], edge_recv.at[gy], a2a_send.at[halves], a2a_recv.at[halves],
                 (gx, peer(i))).start()

    block_drains = [
        drain(recv[h].at[0 : ny - 1], a2a_send.at[h], a2a_recv.at[h]) for h in range(halves)
    ]
    edge_drain = drain(edge_recv.at[0 : ny - 1], a2a_send.at[halves], a2a_recv.at[halves])

    turn(0)
    fill(0)
    site_lane = lax.broadcasted_iota(jnp.int32, (2, wide, BLOCK), 2)
    site_row = lax.broadcasted_iota(jnp.int32, (2, wide, BLOCK), 1)
    span = 4 * HALO
    low = site_lane < BLOCK // 2
    keep_own = vacancy_ref[...].astype(F32)
    ends = []
    for own in (disorder_ref[...], keep_own):
        ends.append(jnp.where(low, own[:, :, 0:BLOCK], own[:, :, long - BLOCK : long]))
    keep_end = jnp.where(low, pltpu.roll(ends[1], HALO, axis=2),
                         pltpu.roll(ends[1], BLOCK - HALO, axis=2))
    packed = jnp.where(((site_lane + HALO) & (BLOCK - 1)) < 2 * HALO, ends[0], keep_end)
    packed = pltpu.roll(packed, 0, axis=2, stride=span, stride_axis=1)
    packed = jnp.where(((site_lane + span // 2) & (BLOCK - 1)) // span == site_row, packed, 0.0)
    site_edge[...] = jnp.sum(packed, axis=1, keepdims=True)
    for a in (-1, 1):
        kept = rows_to(a, wide)
        rows = (disorder_ref[:, kept, :], keep_own[:, kept, :])
        site_send_x[0 if a == -1 else 1] = jnp.concatenate(rows, axis=1)
    sites = {}

    def site(name, source, target, w, device, when=None):
        sites[name] = copy(source, target, site_send.at[w], site_recv.at[w], device)
        if when is None:
            sites[name].start()
        else:
            pl.when(when)(sites[name].start)

    x_drain = drain(site_x, site_send.at[0], site_recv.at[0])
    y_drain = drain(site_y, site_send.at[1], site_recv.at[1])
    z_drain = drain(site_z, site_send.at[2], site_recv.at[2])

    for h in range(1, halves):
        turn(h)
    fill_edges()
    pl.semaphore_wait(barrier, entered)
    start_edges()
    pass_on(0)
    for side, a in enumerate((-1, 1)):
        site(("x", a), site_send_x.at[side], site_x.at[side], 0, at(a, 0), linked[a])
        site(("y", a), site_edge, site_y.at[side], 1, at(0, a))
    start_blocks(0)

    def token_round(step):
        hear(step)
        if step < nx - 2:
            pass_on(step + 1)

    for step in range(nx - 3):
        token_round(step)
    for h in range(1, halves):
        fill(h)
        block_drains[h - 1].wait_send()
        if h == final:
            token_round(nx - 3)
            for a in (-1, 1):
                pl.when(~linked[a])(sites["x", a].start)
        start_blocks(h)

    short = lax.broadcasted_iota(jnp.int32, (2, 1, BLOCK), 2)

    def site_ends(a, both):
        rows, kept = rows_from(a, wide), rows_to(a, wide)
        for x in range(rows.start, rows.stop):
            shift = 2 * BLOCK - span * (x - rows.start + kept.start)
            energy = pltpu.roll(both, shift % BLOCK, axis=2)
            present = jnp.where(short < BLOCK // 2,
                                pltpu.roll(both, (shift - HALO) % BLOCK, axis=2),
                                pltpu.roll(both, (shift + HALO) % BLOCK, axis=2))
            scale = present * (1.0 / SPREAD)
            keep_ref[:, x : x + 1, long:] = present
            factor[:, x : x + 1, long:] = scale
            onsite[:, x : x + 1, long:] = energy * scale

    def site_rows(a, energy, present):
        rows = rows_from(a, wide)
        scale = present * (1.0 / SPREAD)
        keep_ref[:, rows, 0:long] = present
        factor[:, rows, 0:long] = scale
        onsite[:, rows, 0:long] = energy * scale

    site_rows(0, disorder_ref[...], keep_own)
    y_drain.wait()
    site_both[...] = jnp.where((short & (span // 2)) == 0, site_y[0], site_y[1])
    for side, a in enumerate((-1, 1)):
        site(("z", a), site_both, site_z.at[side], 2, at(a, 0))
    site_ends(0, site_both[...])

    def far_sites():
        x_drain.wait()
        z_drain.wait()
        for side, a in enumerate((-1, 1)):
            site_rows(a, site_x[side, :, 0:HALO], site_x[side, :, HALO:])
            site_ends(a, site_z[side])

    def begin(h, first, last, edges):
        for x in range(first, last):
            rows = lattice[h, x].astype(F32)
            shift = (-2 * HALO * (h * wide + edges[1] + x - first)) % BLOCK
            edge = pltpu.roll(edges[0], shift, axis=1) if shift else edges[0]
            for s in range(2):
                mask = keep_ref[s, x : x + 1, :]
                own = slice(s * GROUP, (s + 1) * GROUP)
                real0[h, s, x, :, 0:long] = rows[own] * mask[:, 0:long]
                real0[h, s, x, :, long:] = edge[own] * mask[:, long:]

    near_drains = [
        drain(lattice.at[h, 0 : 2 * NEAR], halo_send.at[h, 0], halo_recv.at[h, 0])
        for h in range(halves)
    ]
    far_drains = [
        drain(lattice.at[h, 0 : 2 * NEAR], halo_send.at[h, 1], halo_recv.at[h, 1])
        for h in range(halves)
    ]
    inner = linked[-1] & linked[1]
    one_drain = drain(lattice.at[final, 0:NEAR], halo_send.at[final, 0], halo_recv.at[final, 0])
    direct_drain = drain(near_in, direct_send.at[0], direct_recv.at[0])
    side_drain = drain(edge_side, halo_send.at[0, 2], halo_recv.at[0, 2])

    def halo(h, a, source, target, slot, when=None):
        move = copy(source, target, halo_send.at[h, slot], halo_recv.at[h, slot], at(a, 0))
        if when is None:
            move.start()
        else:
            pl.when(when)(move.start)

    def own_edge():
        left = plan_ref[lax.rem(gy * blocks - 1 + ny * blocks, ny * blocks)] // blocks
        right = plan_ref[lax.rem(gy * blocks + blocks, ny * blocks)] // blocks
        return jnp.where(is_last, edge_recv[left].astype(F32), edge_recv[right].astype(F32))

    def send_rows(h, name):
        for a in (1, -1):
            last = (a == 1) == (name == "near")
            cut = slice(HALO - NEAR, HALO) if last else slice(0, NEAR)
            rows_out, rows_in = rows_to(a, wide).start + HALO, rows_from(a, wide).start
            source = lattice.at[h, rows_out + cut.start : rows_out + cut.stop]
            target = lattice.at[h, rows_in + cut.start : rows_in + cut.stop]
            relayed = linked[a] if h == final and name == "near" else None
            halo(h, a, source, target, 0 if name == "near" else 1, relayed)

    def arrive(h):
        block_drains[h].wait_recv()
        if h == halves - 1:
            block_drains[h].wait_send()
        for k in range(blocks):
            source = plan_ref[gy * blocks + k] // blocks
            lattice[h, HALO : HALO + wide, :, k * BLOCK : (k + 1) * BLOCK] = recv[h][source]
        send_rows(h, "near")
        if h == 0:
            edge_drain.wait()
            edge_own[...] = own_edge().astype(BF16)
            for a in (1, -1):
                halo(0, a, edge_own, edge_side.at[0 if a == -1 else 1], 2)
        if h == 0:
            token_round(nx - 2)
            for a in (-1, 1):
                pl.when(~linked[a])(functools.partial(start_direct, a))
        begin(h, HALO, HALO + wide, (own_edge(), 0))

    def back(value):
        return pltpu.roll(value, 1, axis=1)

    def ahead(value):
        return pltpu.roll(value, extent - 1, axis=1)

    def bond(r, i, first, second, chiral, want_imag):
        turn = chiral * sin
        out_real = cos * (r[first] + r[second])
        if i is not None:
            out_real = out_real - turn * (i[first] - i[second])
        out_imag = None
        if want_imag:
            out_imag = turn * (r[first] - r[second])
            if i is not None:
                out_imag = out_imag + cos * (i[first] + i[second])
        return out_real, out_imag

    reals_of = (real0, real1, real2, real3)
    imags_of = (None, imag1, imag2, imag3)

    def term(n, h, count, where, measure):
        if count <= 0:
            return
        cur_r, cur_i = reals_of[n - 1], imags_of[n - 1]
        complex_in, want_imag, keep_new = n > 1, n < TERMS, n < TERMS

        def row(x, measured):
            reals = [[cur_r[h, s, x + d] for d in (-1, 0, 1)] for s in range(2)]
            imags = [None, None]
            if complex_in:
                imags = [[cur_i[h, s, x + d] for d in (-1, 0, 1)] for s in range(2)]
            for s, chiral in ((0, 1.0), (1, -1.0)):
                r, i = reals[s], imags[s]
                other_r, other_i = reals[1 - s], imags[1 - s]
                here = bond(r, i, 2, 0, chiral, want_imag)
                behind = bond(r, i, 1, 2, chiral, want_imag)
                front = bond(r, i, 0, 1, chiral, want_imag)
                level = onsite[s, pl.ds(x, 1), :]
                scale = factor[s, pl.ds(x, 1), :]
                if n > 1:
                    level, scale = 2.0 * level, 2.0 * scale
                away = 0 if s == 0 else 2
                results = []
                for part_of in range(2 if want_imag else 1):
                    own, other = (r, other_r) if part_of == 0 else (i, other_i)
                    hop, prior, later = here[part_of], behind[part_of], front[part_of]
                    if other is not None:
                        hop = hop - (other[1] + other[away])
                        if s == 0:
                            prior = prior - other[1]
                        else:
                            later = later - other[1]
                    result = (hop + (back(prior) + ahead(later))) * scale
                    if own is not None:
                        result = result + level * own[1]
                    fields = reals_of if part_of == 0 else imags_of
                    if n > 1 and fields[n - 2] is not None:
                        result = result - fields[n - 2][h, s, x]
                    if keep_new:
                        fields[n][h, s, x] = result
                    results.append(result[:, :long])
                if measured is not None:
                    measured(s, x, real0[h, s, x, :, 0:long], results,
                             r[1][:, :long], None if i is None else i[1][:, :long])

        def plain(t, carry):
            row(where(t), None)
            return carry

        def middle(t, carry):
            def measured(s, x, start, results, now_r, now_i):
                product = start * results[0]
                total = product
                if h > 0:
                    total = sums[n - 1, s, x - HALO] + product
                if h < halves - 1:
                    sums[n - 1, s, x - HALO] = total
                else:
                    moments_ref[n - 1, s, pl.ds(x - HALO, 1), :] = (
                        jnp.sum(total, axis=0, keepdims=True) * (1.0 / vectors))
                if n == 1:
                    extra = ((0, product), (4, start * start))
                elif n == 2:
                    extra = (
                        (1, product),
                        (2, now_r * results[0] + now_i * results[1]),
                        (3, results[0] * results[0] + results[1] * results[1]),
                    )
                else:
                    extra = ()
                for slot, value in extra:
                    total = traces[h, slot]
                    for k in range(blocks):
                        total = total + value[:, k * BLOCK : (k + 1) * BLOCK]
                    traces[h, slot] = total

            row(where(t), measured)
            return carry

        lax.fori_loop(0, count, middle if measure else plain, 0, unroll=True)

    def inside(n, h):
        term(n, h, wide - 2 * n, lambda t: HALO + n + t, True)

    def border(n, h):
        term(n, h, 2 * n, lambda t: HALO + t + (wide - 2 * n) * (t // n), True)

    def halo_edges():
        return {a: edge_side[0 if a == -1 else 1].astype(F32) for a in (1, -1)}

    def near_stage(h):
        if h == 0:
            side_drain.wait()
        if h < final:
            near_drains[h].wait()
        else:
            pl.when(inner)(near_drains[h].wait_recv)
            pl.when(~inner)(one_drain.wait_recv)
            pl.when(~inner)(direct_drain.wait)

            def land(start):
                for k in range(blocks):
                    source = plan_ref[gy * blocks + k] // blocks
                    lattice[h, start : start + NEAR, :, k * BLOCK : (k + 1) * BLOCK] = near_in[source]

            pl.when(~linked[-1])(functools.partial(land, HALO - NEAR))
            pl.when(~linked[1])(functools.partial(land, HALO + wide))
        edges = halo_edges()
        begin(h, HALO - NEAR, HALO, (edges[1], wide - NEAR))
        begin(h, HALO + wide, HALO + wide + NEAR, (edges[-1], 0))
        term(1, h, 2, lambda t: HALO - 1 + t * (wide + 1), False)
        border(1, h)
        border(2, h)

    def far_stage(h):
        far_drains[h].wait()
        edges = halo_edges()
        begin(h, 0, HALO - NEAR, (edges[1], wide - HALO))
        begin(h, HALO + wide + NEAR, 2 * HALO + wide, (edges[-1], NEAR))
        term(1, h, 4, lambda t: 1 + t + (t // 2) * (wide + 2), False)
        term(2, h, 4, lambda t: 2 + t + (t // 2) * wide, False)
        term(3, h, 2, lambda t: 3 + t * (wide + 1), False)
        border(3, h)
        term(TERMS, h, wide, lambda t: HALO + t, True)

    small = lax.broadcasted_iota(jnp.int32, (GROUP, BLOCK), 1)
    slot_of = lax.broadcasted_iota(jnp.int32, (GROUP, BLOCK), 0)

    def gather_traces(h):
        out = jnp.zeros((GROUP, BLOCK), F32)
        for n in range(TERMS):
            value = traces[h, n]
            if n == 2:
                value = 2.0 * value - traces[h, 0]
            if n == 3:
                value = 2.0 * value - traces[h, 4]
            total = jnp.sum(value, axis=1, keepdims=True)
            out = jnp.where(small == slot_of + (n * vectors + h * GROUP), total, out)
        return jnp.sum(out, axis=0, keepdims=True)

    trace_row = jnp.zeros((1, BLOCK), F32)
    for h in range(halves):
        arrive(h)
        if h == final:
            for later in range(halves):
                send_rows(later, "far")
        for n in range(1, TERMS):
            inside(n, h)
    far_sites()
    pl.when(inner)(near_drains[final].wait_send)
    pl.when(~inner)(one_drain.wait_send)
    for h in range(halves):
        near_stage(h)
        trace_row = trace_row + gather_traces(h)
    part[...] = trace_row
    me = gx * ny + gy
    parts[me] = trace_row
    for i in range(1, many):
        copy(part, parts.at[me], sum_send.at[0], sum_recv.at[0], at(i // ny, i % ny)).start()
    for h in range(halves):
        far_stage(h)
    drain(parts.at[0 : many - 1], sum_send.at[0], sum_recv.at[0]).wait()
    total = parts[0]
    for p in range(1, many):
        total = total + parts[p]
    sites_total = 2 * wide * nx * long * ny
    total = total * (1.0 / sites_total)
    for n in range(TERMS):
        turned_row = pltpu.roll(total, BLOCK - n * vectors, axis=1) if n else total
        trace_ref[n : n + 1, :] = turned_row[:, :vectors]


def store(moments_ref, trace_ref, moments_any, trace_any, sems):
    copies = [
        pltpu.make_async_copy(trace_ref, trace_any, sems.at[0]),
        pltpu.make_async_copy(moments_ref, moments_any, sems.at[1]),
    ]
    for move in copies:
        move.start()
    for move in copies:
        move.wait()


def local(nx, ny, stored_vectors, disorder, vacancy, plan):
    vectors, wide, long = stored_vectors.shape[1:]
    tall, extent = wide + 2 * HALO, long + BLOCK
    halves, blocks, pair = vectors // GROUP, long // BLOCK, 2 * GROUP
    dma = pltpu.SemaphoreType.DMA
    many = nx * ny
    field = pltpu.VMEM((halves, 2, tall, GROUP, extent), F32)
    moments, trace = pl.pallas_call(
        functools.partial(program, nx, ny),
        out_shape=(
            pltpu.VMEM((TERMS, 2, wide, long), F32),
            pltpu.VMEM((TERMS, vectors), F32),
        ),
        in_specs=[pl.BlockSpec(memory_space=pl.ANY)] * 4,
        out_specs=(pl.BlockSpec(memory_space=pltpu.VMEM),) * 2,
        scratch_shapes=[
            pltpu.SMEM(plan.shape, jnp.int32),
            pltpu.VMEM(stored_vectors.shape, BF16),
            pltpu.VMEM(disorder.shape, F32),
            pltpu.VMEM(vacancy.shape, jnp.int32),
            pltpu.VMEM((halves, blocks, wide, pair, BLOCK), BF16),
            pltpu.VMEM((blocks, pair, BLOCK), F32),
            pltpu.VMEM((halves, ny, wide, pair, BLOCK), BF16),
            pltpu.VMEM((ny, pair, BLOCK), BF16),
            pltpu.VMEM((ny, pair, BLOCK), BF16),
            pltpu.VMEM((halves, tall, pair, long), BF16),
            pltpu.VMEM((pair, BLOCK), BF16),
            pltpu.VMEM((2, pair, BLOCK), BF16),
            pltpu.VMEM((2, 2, 2 * HALO, long), F32),
            pltpu.VMEM((2, 2, 2 * HALO, long), F32),
            pltpu.VMEM((2, 1, BLOCK), F32),
            pltpu.VMEM((2, 2, 1, BLOCK), F32),
            pltpu.VMEM((2, 1, BLOCK), F32),
            pltpu.VMEM((2, 2, 1, BLOCK), F32),
        ]
        + [pltpu.VMEM((2, tall, extent), F32)] * 3
        + [field] * 7
        + [
            pltpu.VMEM((TERMS, 2, wide, GROUP, long), F32),
            pltpu.VMEM((halves, TERMS + 1, GROUP, BLOCK), F32),
            pltpu.VMEM((1, BLOCK), F32),
            pltpu.VMEM((many, 1, BLOCK), F32),
            dma((4,)),
            dma((halves + 1,)), dma((halves + 1,)),
            dma((halves, 3)), dma((halves, 3)),
            dma((3,)), dma((3,)),
            dma((1,)), dma((1,)),
            dma((1,)), dma((1,)),
            pltpu.SemaphoreType.REGULAR((nx - 1, 2)),

        ]
        + [pltpu.VMEM((ny, wide, pair, BLOCK), BF16)] * halves
        + [pltpu.VMEM((ny, NEAR, pair, BLOCK), BF16)],
        compiler_params=pltpu.CompilerParams(collective_id=0, has_side_effects=True),
        name="chebyshev",
    )(plan, stored_vectors, disorder, vacancy)
    moments = pltpu.with_memory_space_constraint(moments, pltpu.VMEM)
    trace = pltpu.with_memory_space_constraint(trace, pltpu.VMEM)
    return pl.pallas_call(
        store,
        out_shape=(
            jax.ShapeDtypeStruct(moments.shape, F32),
            jax.ShapeDtypeStruct(trace.shape, F32),
        ),
        in_specs=[pl.BlockSpec(memory_space=pltpu.VMEM)] * 2,
        out_specs=(pl.BlockSpec(memory_space=pl.ANY),) * 2,
        scratch_shapes=[dma((2,))],
        name="store",
    )(moments, trace)


def solution(mesh):
    placed = (P(None, None, "gx", "gy"), P(None, "gx", "gy"), P(None, "gx", "gy"), P())
    return jax.shard_map(
        functools.partial(local, mesh.shape["gx"], mesh.shape["gy"]),
        mesh=mesh,
        in_specs=placed,
        out_specs=(P(None, None, "gx", "gy"), P()),
        check_vma=False,
    )
```
